32 devices in a mesh: stack: 2 (over y), date: 4 (over x, core), line: 4 (over z).
Axes of the slice: x: 2, y: 2, z: 4, core: 2. Of those that a mesh axis runs over, the one named last changes fastest.
Arguments:
- slc: float32 [4, 2, 512, 1280], P('date', None, 'stack', 'line'), parts along dimension 2, may hold values from -6 to 6
- band_start: int32 [4], replicated, may hold values from 0 to 640, as said below
- band_stop: int32 [4], replicated, may hold values from 640 to 1280, as said below
Outputs:
- interferogram: float32 [4, 2, 512, 256], P('date', None, 'stack', 'line'), parts along dimension 2
The draws below stay inside these ranges and needn't reach their ends.
There are 2 independent parts, one for each index of `stack`. The reference program is written for one: setup_inputs(seed, part) draws one part's arguments, and reference() takes and returns one part's arrays. A program takes and returns all parts, laid end to end along the dimension named above; an argument that names none is the same for every part. Nothing has to cross between parts.
Inputs may be any that keep to these rules, and one draw needn't show every extreme that they name: For every pair, band_stop - band_start lies between 640 and 960; at least one pair keeps exactly 960 bins, and some pair keeps exactly 640 bins ending at 1280. `band_stop`: see band_start.
All inputs are finite; a program needn't handle non-finite values.
Results may differ from the reference program's by a relative error of at most 0.0001.
Values sent between devices are 32-bit elements; how exact they have to be, the bound alone decides.
No kernel may reach another device: no remote copies, remote signals or barrier semaphores. Data moves between devices by JAX's collectives and lax.ppermute only.
A program may use at most 64 MiB of HBM per device.

```python
import jax
import jax.numpy as jnp

COLS = 256
LOOKS = 5
LINES = 1280
DATES = 4


def band_pair(key):
    key_width = jax.random.fold_in(key, 11)
    key_chosen = jax.random.fold_in(key, 23)
    key_offset = jax.random.fold_in(key, 37)
    narrowest = LINES // 2
    widest = 3 * LINES // 4
    order = jax.random.permutation(key_chosen, jnp.arange(DATES, dtype=jnp.int32))
    pair_ids = jnp.arange(DATES, dtype=jnp.int32)
    widths = jax.random.randint(key_width, (DATES,), narrowest, widest + 1)
    widths = jnp.where(pair_ids == order[0], widest, widths)
    widths = jnp.where((pair_ids == order[1]) | (pair_ids == order[2]), narrowest, widths)
    starts = jax.random.randint(key_offset, (DATES,), 0, LINES - widths + 1)
    starts = jnp.where(pair_ids == order[1], LINES - narrowest, starts)
    starts = jnp.where(pair_ids == order[2], 0, starts)
    return (starts.astype(jnp.int32), (starts + widths).astype(jnp.int32))


def draw_band_start(key, part):
    return band_pair(key)[0]


def draw_band_stop(key, part):
    return band_pair(key)[1]


def steps_of(own_key, shape, split, least, largest):
    factor_of, own = 1.0, jax.random.fold_in(own_key, 6)
    for dim, parts in split:
        steps = jnp.exp(jax.random.uniform(jax.random.fold_in(own, dim), (parts,), jnp.float32, least / len(split), largest / len(split)))
        factor_of = factor_of * jnp.repeat(steps, shape[dim] // parts).reshape([-1 if axis == dim else 1 for axis in range(len(shape))])
    return factor_of


def normal_values(key, dims, width, bound, pieces=(), kind=jnp.bfloat16):
    gain = steps_of(key, dims, pieces, -0.22, 0.18) if pieces else 1.0
    drawn = jax.random.normal(key, dims, jnp.float32) * width * gain
    return jnp.minimum(jnp.maximum(drawn, -bound), bound).astype(kind)


def setup_inputs(seed: int = 0, part: int = 0) -> dict:
    key_of = jax.random.split(jax.random.key(seed), 4)
    part_splits = jax.random.split(jax.random.fold_in(key_of[3], part), 4)
    return {
        "slc": normal_values(part_splits[0], (DATES, 2, COLS, LINES), 1.0, 6.0, ((0, 4), (3, 4)), jnp.float32),
        "band_start": draw_band_start(jax.random.fold_in(key_of[3], 71), part),
        "band_stop": draw_band_stop(jax.random.fold_in(key_of[3], 71), part),
    }


def reference(slc, band_start, band_stop):
    images = slc[:, 0] + 1j * slc[:, 1]
    spectra = jnp.fft.fft(images, axis=-1)
    partner = jnp.roll(spectra, -1, axis=0)
    bins_all = jnp.arange(LINES, dtype=jnp.int32)
    keep_mask = (bins_all[None, :] >= band_start[:, None]) & (bins_all[None, :] < band_stop[:, None])
    keep_mask = keep_mask[:, None, :]
    ref_signal = jnp.fft.ifft(jnp.where(keep_mask, spectra, 0), axis=-1)
    sec_signal = jnp.fft.ifft(jnp.where(keep_mask, partner, 0), axis=-1)
    product = ref_signal * jnp.conj(sec_signal)
    looked = product.reshape(DATES, COLS, LINES // LOOKS, LOOKS).mean(axis=-1)
    return jnp.stack([jnp.real(looked), jnp.imag(looked)], axis=1).astype(jnp.float32)
```

```python
import functools
import math

import jax
import jax.numpy as jnp
import numpy as np
from jax import lax
from jax.experimental import pallas as pl
from jax.experimental.pallas import tpu as pltpu
from jax.sharding import PartitionSpec as P

LOOKS = 5
LANES = 128
MIB = 1 << 20
HALF = LANES // 2


HIGHEST_PRECISION = lax.Precision.HIGHEST


def shifted(shard, axis, by):
    size = lax.axis_size(axis)
    return lax.ppermute(shard, axis, [(i, (i + by) % size) for i in range(size)])


def phase_table(count, sign_value):
    index_row = jnp.arange(count, dtype=jnp.int32)
    wrapped = index_row[:, None] * index_row[None, :] % count
    angle_all = 2.0 * math.pi / count * wrapped.astype(jnp.float32)
    return (jnp.cos(angle_all), sign_value * jnp.sin(angle_all))


def twiddle_table(outer, inner, sign_value):
    outer_row = jnp.arange(outer, dtype=jnp.int32)
    inner_row = jnp.arange(inner, dtype=jnp.int32)
    wrapped = outer_row[:, None] * inner_row[None, :] % (outer * inner)
    angle_all = 2.0 * math.pi / (outer * inner) * wrapped.astype(jnp.float32)
    return (jnp.cos(angle_all), sign_value * jnp.sin(angle_all))


def left_product(table_real, table_imag, data_real, data_imag):

    def single(table, data):
        return jnp.einsum("ka,cab->ckb", table, data, precision=HIGHEST_PRECISION)

    return (
        single(table_real, data_real) - single(table_imag, data_imag),
        single(table_real, data_imag) + single(table_imag, data_real),
    )


def right_product(data_real, data_imag, table_real, table_imag):

    def single(data, table):
        return jnp.einsum("ckb,bm->ckm", data, table, precision=HIGHEST_PRECISION)

    return (
        single(data_real, table_real) - single(data_imag, table_imag),
        single(data_imag, table_real) + single(data_real, table_imag),
    )


def forward_dft(data_real, data_imag):
    outer = data_real.shape[1]
    inner = data_real.shape[2]
    outer_real, outer_imag = phase_table(outer, -1.0)
    first_real, first_imag = left_product(outer_real, outer_imag, data_real, data_imag)
    twist_real, twist_imag = twiddle_table(outer, inner, -1.0)
    turned_real = first_real * twist_real - first_imag * twist_imag
    turned_imag = first_real * twist_imag + first_imag * twist_real
    inner_real, inner_imag = phase_table(inner, -1.0)
    return right_product(turned_real, turned_imag, inner_real, inner_imag)


def inverse_dft(data_real, data_imag):
    outer = data_real.shape[1]
    inner = data_real.shape[2]
    inner_real, inner_imag = phase_table(inner, 1.0)
    first_real, first_imag = right_product(data_real, data_imag, inner_real, inner_imag)
    twist_real, twist_imag = twiddle_table(outer, inner, 1.0)
    turned_real = first_real * twist_real - first_imag * twist_imag
    turned_imag = first_real * twist_imag + first_imag * twist_real
    outer_real, outer_imag = phase_table(outer, 1.0)
    result_real, result_imag = left_product(outer_real, outer_imag, turned_real, turned_imag)
    scale = 1.0 / (outer * inner)
    return (result_real * scale, result_imag * scale)


def conj_product(ref_real, ref_imag, sec_real, sec_imag):
    return (ref_real * sec_real + ref_imag * sec_imag, ref_imag * sec_real - ref_real * sec_imag)


def look_mean(values):
    return values.reshape(values.shape[0], values.shape[1] // LOOKS, LOOKS).sum(axis=-1) * (
        1.0 / LOOKS
    )


def general_shards(slc, band_start, band_stop):
    own_image = slc[0]
    line_lines = own_image.shape[2]
    turned = lax.all_to_all(own_image, "line", split_axis=1, concat_axis=2, tiled=True)
    columns = turned.shape[1]
    outer = lax.axis_size("line")
    lines_all = outer * line_lines
    blocks = turned.reshape(2, columns, outer, line_lines)
    spec_real, spec_imag = forward_dft(blocks[0], blocks[1])
    spectrum = jnp.stack([spec_real, spec_imag], axis=0)
    date_index = lax.axis_index("date")
    my_start = lax.dynamic_slice_in_dim(band_start, date_index, 1)[0]
    my_end = lax.dynamic_slice_in_dim(band_stop, date_index, 1)[0]
    bin_index = (
        jnp.arange(outer, dtype=jnp.int32)[:, None]
        + outer * jnp.arange(line_lines, dtype=jnp.int32)[None, :]
    )
    keep_mask = ((bin_index >= my_start) & (bin_index < my_end)).astype(jnp.float32)
    partner = shifted(spectrum, "date", -1)
    ref_spec = spectrum * keep_mask
    sec_spec = partner * keep_mask
    both_real, both_imag = inverse_dft(
        jnp.concatenate([ref_spec[0], sec_spec[0]], axis=0),
        jnp.concatenate([ref_spec[1], sec_spec[1]], axis=0),
    )
    ref_real = both_real[:columns].reshape(columns, lines_all)
    ref_imag = both_imag[:columns].reshape(columns, lines_all)
    sec_real = both_real[columns:].reshape(columns, lines_all)
    sec_imag = both_imag[columns:].reshape(columns, lines_all)
    prod_real, prod_imag = conj_product(ref_real, ref_imag, sec_real, sec_imag)
    looked = jnp.stack([look_mean(prod_real), look_mean(prod_imag)], axis=0)
    result = lax.all_to_all(looked, "line", split_axis=2, concat_axis=1, tiled=True)
    return result[None]


def split_pair(values):
    high = values.astype(jnp.bfloat16)
    low = (values - high.astype(jnp.float32)).astype(jnp.bfloat16)
    return high, low


@functools.lru_cache(maxsize=None)
def host_tables(inner):
    index = np.arange(inner)
    angle = 2.0 * np.pi * ((index[:, None] * index[None, :]) % inner) / inner
    both = np.concatenate([np.cos(angle), np.sin(angle)], axis=1)
    high = both.astype(jnp.bfloat16)
    low = (both - high.astype(np.float64)).astype(jnp.bfloat16)
    matrix = np.stack([high, low])
    turn = 2.0 * np.pi * np.arange(1, LOOKS)[:, None] * index[None, :] / (LOOKS * inner)
    twist = np.stack([np.cos(turn), np.sin(turn)], axis=1).astype(np.float32)
    twist = np.broadcast_to(twist[..., None], (LOOKS - 1, 2, inner, LANES))
    return matrix, np.ascontiguousarray(twist)


def low_lanes(shape):
    return lax.broadcasted_iota(jnp.int32, shape, len(shape) - 1) < HALF


def swap_halves(values):
    return pltpu.roll(values, HALF, values.ndim - 1)


def pack_kernel(peers, image_ref, *chunk_refs):
    me = lax.axis_index("line")
    side = me % 2
    for pair in range(peers // 2):
        block = jnp.bitwise_xor(me // 2, pair)
        lane = pl.multiple_of(block * LANES, LANES)
        real = image_ref[0, :, pl.ds(lane, LANES)]
        imag = image_ref[1, :, pl.ds(lane, LANES)]
        mask = low_lanes(real.shape)
        first = jnp.where(mask, real, swap_halves(imag))
        second = jnp.where(mask, swap_halves(real), imag)
        chunk_refs[2 * pair][...] = jnp.where(side == 0, first, second)
        chunk_refs[2 * pair + 1][...] = jnp.where(side == 0, second, first)


COS1, COS2 = math.cos(2.0 * math.pi / 5), math.cos(4.0 * math.pi / 5)
SIN1, SIN2 = math.sin(2.0 * math.pi / 5), math.sin(4.0 * math.pi / 5)


def five_point(real, imag, sign):
    sum_r1, sum_i1 = real[1] + real[4], imag[1] + imag[4]
    sum_r2, sum_i2 = real[2] + real[3], imag[2] + imag[3]
    dif_r1, dif_i1 = real[1] - real[4], imag[1] - imag[4]
    dif_r2, dif_i2 = real[2] - real[3], imag[2] - imag[3]
    out_r0, out_i0 = real[0] + sum_r1 + sum_r2, imag[0] + sum_i1 + sum_i2
    even_r1 = real[0] + COS1 * sum_r1 + COS2 * sum_r2
    even_i1 = imag[0] + COS1 * sum_i1 + COS2 * sum_i2
    even_r2 = real[0] + COS2 * sum_r1 + COS1 * sum_r2
    even_i2 = imag[0] + COS2 * sum_i1 + COS1 * sum_i2
    odd_r1 = (sign * SIN1) * dif_r1 + (sign * SIN2) * dif_r2
    odd_i1 = (sign * SIN1) * dif_i1 + (sign * SIN2) * dif_i2
    odd_r2 = (sign * SIN2) * dif_r1 - (sign * SIN1) * dif_r2
    odd_i2 = (sign * SIN2) * dif_i1 - (sign * SIN1) * dif_i2
    return (
        [out_r0, even_r1 - odd_i1, even_r2 - odd_i2, even_r2 + odd_i2, even_r1 + odd_i1],
        [out_i0, even_i1 + odd_r1, even_i2 + odd_r2, even_i2 - odd_r2, even_i1 - odd_r1],
    )


def main_kernel(peers, inner, start_ref, stop_ref, matrix_ref, twist_ref, *refs):
    own_refs, sec_refs = refs[:peers], refs[peers : 2 * peers]
    out_refs = refs[2 * peers : 3 * peers]
    real_ref, imag_ref, mid_ref, high_ref, low_ref, sum_ref = refs[3 * peers :]
    me = lax.axis_index("line")
    date = lax.axis_index("date")
    chunk_lines = own_refs[0].shape[0]
    lines_all = peers * chunk_lines
    for r in range(peers):
        base = pl.multiple_of(jnp.bitwise_xor(me, r) * chunk_lines, 8)
        own, sec = own_refs[r][...], sec_refs[r][...]
        mask = low_lanes(own.shape)
        real_ref[pl.ds(base, chunk_lines), :] = jnp.where(mask, own, swap_halves(sec))
        imag_ref[pl.ds(base, chunk_lines), :] = jnp.where(mask, swap_halves(own), sec)

    high_table, low_table = matrix_ref[0], matrix_ref[1]

    def transform(high, low):
        return (
            jnp.dot(high_table, high, preferred_element_type=jnp.float32)
            + jnp.dot(high_table, low, preferred_element_type=jnp.float32)
            + jnp.dot(low_table, high, preferred_element_type=jnp.float32)
        )

    for l in range(LOOKS):
        real_high, real_low = split_pair(real_ref[pl.ds(l, inner, stride=LOOKS), :])
        imag_high, imag_low = split_pair(imag_ref[pl.ds(l, inner, stride=LOOKS), :])
        high = jnp.concatenate(
            [
                jnp.concatenate([real_high, imag_high], axis=1),
                jnp.concatenate([imag_high, -real_high], axis=1),
            ],
            axis=0,
        )
        low = jnp.concatenate(
            [
                jnp.concatenate([real_low, imag_low], axis=1),
                jnp.concatenate([imag_low, -real_low], axis=1),
            ],
            axis=0,
        )
        mid_ref[l] = transform(high, low)

    start, stop = start_ref[date], stop_ref[date]
    rows = 16

    def spectral(step, carry):
        row = pl.multiple_of(step * rows, rows)
        span = pl.ds(row, rows)
        real = [mid_ref[l, span, :LANES] for l in range(LOOKS)]
        imag = [mid_ref[l, span, LANES:] for l in range(LOOKS)]
        turn = [(twist_ref[l, 0, span, :], twist_ref[l, 1, span, :]) for l in range(LOOKS - 1)]
        for l in range(1, LOOKS):
            c, s = turn[l - 1]
            real[l], imag[l] = real[l] * c + imag[l] * s, imag[l] * c - real[l] * s
        real, imag = five_point(real, imag, -1.0)
        first = lax.broadcasted_iota(jnp.int32, (rows, LANES), 0) + row
        for m in range(LOOKS):
            bin_index = first + m * inner
            keep = (bin_index >= start) & (bin_index < stop)
            weight = jnp.where(keep, 1.0 / lines_all, 0.0)
            real[m], imag[m] = real[m] * weight, imag[m] * weight
        real, imag = five_point(real, imag, 1.0)
        for l in range(1, LOOKS):
            c, s = turn[l - 1]
            real[l], imag[l] = real[l] * c - imag[l] * s, imag[l] * c + real[l] * s
        span_below = pl.ds(pl.multiple_of(row + inner, rows), rows)
        for l in range(LOOKS):
            real_high, real_low = split_pair(real[l])
            imag_high, imag_low = split_pair(imag[l])
            high_ref[l, span, :LANES] = real_high
            high_ref[l, span, LANES:] = imag_high
            high_ref[l, span_below, :LANES] = -imag_high
            high_ref[l, span_below, LANES:] = real_high
            low_ref[l, span, :LANES] = real_low
            low_ref[l, span, LANES:] = imag_low
            low_ref[l, span_below, :LANES] = -imag_low
            low_ref[l, span_below, LANES:] = real_low
        return carry

    lax.fori_loop(0, inner // rows, spectral, 0)

    total = None
    for l in range(LOOKS):
        signal = transform(high_ref[l], low_ref[l])
        real, imag = signal[:, :LANES], signal[:, LANES:]
        real_other, imag_other = swap_halves(real), swap_halves(imag)
        product = jnp.where(
            low_lanes(real.shape),
            real * real_other + imag * imag_other,
            real * imag_other - imag * real_other,
        )
        total = product if total is None else total + product
    sum_ref[...] = total * (1.0 / LOOKS)
    out_lines = inner // peers
    for r in range(peers):
        base = pl.multiple_of(jnp.bitwise_xor(me, r) * out_lines, 8)
        out_refs[r][...] = sum_ref[pl.ds(base, out_lines), :]


def unpack_kernel(peers, *refs):
    chunk_refs, out_ref = refs[:peers], refs[peers]
    me = lax.axis_index("line")
    side = me % 2
    for pair in range(peers // 2):
        block = jnp.bitwise_xor(me // 2, pair)
        lane = pl.multiple_of(block * LANES, LANES)
        even, odd = chunk_refs[2 * pair][...], chunk_refs[2 * pair + 1][...]
        first = jnp.where(side == 0, even, odd)
        second = jnp.where(side == 0, odd, even)
        mask = low_lanes(first.shape)
        out_ref[0, :, pl.ds(lane, LANES)] = jnp.where(mask, first, swap_halves(second))
        out_ref[1, :, pl.ds(lane, LANES)] = jnp.where(mask, swap_halves(first), second)


def packed_shards(slc, band_start, band_stop):
    peers, dates = lax.axis_size("line"), lax.axis_size("date")
    chunk_lines = slc.shape[3]
    inner = peers * chunk_lines // LOOKS
    out_lines = inner // peers
    f32 = jnp.float32
    vmem = pl.BlockSpec(memory_space=pltpu.VMEM)
    smem = pl.BlockSpec(memory_space=pltpu.SMEM)
    chunk = jax.ShapeDtypeStruct((chunk_lines, LANES), f32)
    image = jnp.transpose(slc[0], (0, 2, 1))
    packed = pl.pallas_call(
        functools.partial(pack_kernel, peers),
        out_shape=[chunk] * peers,
        in_specs=[vmem],
        out_specs=[vmem] * peers,
        compiler_params=pltpu.CompilerParams(vmem_limit_bytes=8 * MIB),
        name="pack",
    )(image)

    def exchange(values, r):
        return lax.ppermute(values, "line", [(i, i ^ r) for i in range(peers)])

    own = list(packed)
    for r in sorted(range(1, peers), key=lambda r: (r == 1, r)):
        own[r] = exchange(packed[r], r)
    sec = [shifted(values, "date", -1) for values in own]
    matrix, twist = host_tables(inner)
    looked = pl.pallas_call(
        functools.partial(main_kernel, peers, inner),
        out_shape=[jax.ShapeDtypeStruct((out_lines, LANES), f32)] * peers,
        in_specs=[smem, smem, vmem, vmem] + [vmem] * (2 * peers),
        out_specs=[vmem] * peers,
        scratch_shapes=[
            pltpu.VMEM((peers * chunk_lines, LANES), f32),
            pltpu.VMEM((peers * chunk_lines, LANES), f32),
            pltpu.VMEM((LOOKS, inner, 2 * LANES), f32),
            pltpu.VMEM((LOOKS, 2 * inner, 2 * LANES), jnp.bfloat16),
            pltpu.VMEM((LOOKS, 2 * inner, 2 * LANES), jnp.bfloat16),
            pltpu.VMEM((inner, LANES), f32),
        ],
        compiler_params=pltpu.CompilerParams(vmem_limit_bytes=24 * MIB),
        name="interfere",
    )(band_start, band_stop, jnp.asarray(matrix), jnp.asarray(twist), *own, *sec)
    looked = [values if r == 0 else exchange(values, r) for r, values in enumerate(looked)]
    result = pl.pallas_call(
        functools.partial(unpack_kernel, peers),
        out_shape=jax.ShapeDtypeStruct((2, out_lines, slc.shape[2]), f32),
        in_specs=[vmem] * peers,
        out_specs=vmem,
        compiler_params=pltpu.CompilerParams(vmem_limit_bytes=8 * MIB),
        name="unpack",
    )(*looked)
    return jnp.transpose(result, (0, 2, 1))[None]


def packs(mesh, slc):
    peers = mesh.shape["line"]
    columns = slc.shape[2] // mesh.shape["stack"] // peers
    chunk_lines = slc.shape[3] // peers
    inner = slc.shape[3] // LOOKS
    return (
        peers > 1
        and peers & (peers - 1) == 0
        and columns == HALF
        and chunk_lines % 8 == 0
        and inner % (8 * peers) == 0
        and inner % LANES == 0
        and inner <= 4 * LANES
    )


def solution(mesh):
    def whole(slc, band_start, band_stop):
        body = packed_shards if packs(mesh, slc) else general_shards
        return jax.shard_map(
            body,
            mesh=mesh,
            in_specs=(P("date", None, "stack", "line"), P(), P()),
            out_specs=P("date", None, "stack", "line"),
            check_vma=False,
        )(slc, band_start, band_stop)

    return whole
```

```python
import functools
import math

import jax
import jax.numpy as jnp
import numpy as np
from jax import lax
from jax.experimental import pallas as pl
from jax.experimental.pallas import tpu as pltpu
from jax.sharding import PartitionSpec as P


LOOKS = 5
LANES = 128
MIB = 1 << 20
HALF = LANES // 2


HIGHEST_PRECISION = lax.Precision.HIGHEST


def shifted(shard, axis, by):
    size = lax.axis_size(axis)
    return lax.ppermute(shard, axis, [(i, (i + by) % size) for i in range(size)])


def phase_table(count, sign_value):
    index_row = jnp.arange(count, dtype=jnp.int32)
    wrapped = index_row[:, None] * index_row[None, :] % count
    angle_all = 2.0 * math.pi / count * wrapped.astype(jnp.float32)
    return (jnp.cos(angle_all), sign_value * jnp.sin(angle_all))


def twiddle_table(outer, inner, sign_value):
    outer_row = jnp.arange(outer, dtype=jnp.int32)
    inner_row = jnp.arange(inner, dtype=jnp.int32)
    wrapped = outer_row[:, None] * inner_row[None, :] % (outer * inner)
    angle_all = 2.0 * math.pi / (outer * inner) * wrapped.astype(jnp.float32)
    return (jnp.cos(angle_all), sign_value * jnp.sin(angle_all))


def left_product(table_real, table_imag, data_real, data_imag):

    def single(table, data):
        return jnp.einsum("ka,cab->ckb", table, data, precision=HIGHEST_PRECISION)

    return (
        single(table_real, data_real) - single(table_imag, data_imag),
        single(table_real, data_imag) + single(table_imag, data_real),
    )


def right_product(data_real, data_imag, table_real, table_imag):

    def single(data, table):
        return jnp.einsum("ckb,bm->ckm", data, table, precision=HIGHEST_PRECISION)

    return (
        single(data_real, table_real) - single(data_imag, table_imag),
        single(data_imag, table_real) + single(data_real, table_imag),
    )


def forward_dft(data_real, data_imag):
    outer = data_real.shape[1]
    inner = data_real.shape[2]
    outer_real, outer_imag = phase_table(outer, -1.0)
    first_real, first_imag = left_product(outer_real, outer_imag, data_real, data_imag)
    twist_real, twist_imag = twiddle_table(outer, inner, -1.0)
    turned_real = first_real * twist_real - first_imag * twist_imag
    turned_imag = first_real * twist_imag + first_imag * twist_real
    inner_real, inner_imag = phase_table(inner, -1.0)
    return right_product(turned_real, turned_imag, inner_real, inner_imag)


def inverse_dft(data_real, data_imag):
    outer = data_real.shape[1]
    inner = data_real.shape[2]
    inner_real, inner_imag = phase_table(inner, 1.0)
    first_real, first_imag = right_product(data_real, data_imag, inner_real, inner_imag)
    twist_real, twist_imag = twiddle_table(outer, inner, 1.0)
    turned_real = first_real * twist_real - first_imag * twist_imag
    turned_imag = first_real * twist_imag + first_imag * twist_real
    outer_real, outer_imag = phase_table(outer, 1.0)
    result_real, result_imag = left_product(outer_real, outer_imag, turned_real, turned_imag)
    scale = 1.0 / (outer * inner)
    return (result_real * scale, result_imag * scale)


def conj_product(ref_real, ref_imag, sec_real, sec_imag):
    return (ref_real * sec_real + ref_imag * sec_imag, ref_imag * sec_real - ref_real * sec_imag)


def look_mean(values):
    return values.reshape(values.shape[0], values.shape[1] // LOOKS, LOOKS).sum(axis=-1) * (
        1.0 / LOOKS
    )


def general_shards(slc, band_start, band_stop):
    own_image = slc[0]
    line_lines = own_image.shape[2]
    turned = lax.all_to_all(own_image, "line", split_axis=1, concat_axis=2, tiled=True)
    columns = turned.shape[1]
    outer = lax.axis_size("line")
    lines_all = outer * line_lines
    blocks = turned.reshape(2, columns, outer, line_lines)
    spec_real, spec_imag = forward_dft(blocks[0], blocks[1])
    spectrum = jnp.stack([spec_real, spec_imag], axis=0)
    date_index = lax.axis_index("date")
    my_start = lax.dynamic_slice_in_dim(band_start, date_index, 1)[0]
    my_end = lax.dynamic_slice_in_dim(band_stop, date_index, 1)[0]
    bin_index = (
        jnp.arange(outer, dtype=jnp.int32)[:, None]
        + outer * jnp.arange(line_lines, dtype=jnp.int32)[None, :]
    )
    keep_mask = ((bin_index >= my_start) & (bin_index < my_end)).astype(jnp.float32)
    partner = shifted(spectrum, "date", -1)
    ref_spec = spectrum * keep_mask
    sec_spec = partner * keep_mask
    both_real, both_imag = inverse_dft(
        jnp.concatenate([ref_spec[0], sec_spec[0]], axis=0),
        jnp.concatenate([ref_spec[1], sec_spec[1]], axis=0),
    )
    ref_real = both_real[:columns].reshape(columns, lines_all)
    ref_imag = both_imag[:columns].reshape(columns, lines_all)
    sec_real = both_real[columns:].reshape(columns, lines_all)
    sec_imag = both_imag[columns:].reshape(columns, lines_all)
    prod_real, prod_imag = conj_product(ref_real, ref_imag, sec_real, sec_imag)
    looked = jnp.stack([look_mean(prod_real), look_mean(prod_imag)], axis=0)
    result = lax.all_to_all(looked, "line", split_axis=2, concat_axis=1, tiled=True)
    return result[None]


def split_pair(values):
    high = values.astype(jnp.bfloat16)
    low = (values - high.astype(jnp.float32)).astype(jnp.bfloat16)
    return high, low


@functools.lru_cache(maxsize=None)
def host_tables(inner):
    index = np.arange(inner)
    angle = 2.0 * np.pi * ((index[:, None] * index[None, :]) % inner) / inner
    both = np.concatenate([np.cos(angle), np.sin(angle)], axis=1)
    high = both.astype(jnp.bfloat16)
    low = (both - high.astype(np.float64)).astype(jnp.bfloat16)
    matrix = np.stack([high, low])
    turn = 2.0 * np.pi * np.arange(1, LOOKS)[:, None] * index[None, :] / (LOOKS * inner)
    twist = np.stack([np.cos(turn), np.sin(turn)], axis=1).astype(np.float32)
    twist = np.broadcast_to(twist[..., None], (LOOKS - 1, 2, inner, LANES))
    return matrix, np.ascontiguousarray(twist)


def low_lanes(shape):
    return lax.broadcasted_iota(jnp.int32, shape, len(shape) - 1) < HALF


def swap_halves(values):
    return pltpu.roll(values, HALF, values.ndim - 1)


def pack_kernel(peers, image_ref, *chunk_refs):
    me = lax.axis_index("line")
    side = me % 2
    for pair in range(peers // 2):
        block = jnp.bitwise_xor(me // 2, pair)
        lane = pl.multiple_of(block * LANES, LANES)
        real = image_ref[0, :, pl.ds(lane, LANES)]
        imag = image_ref[1, :, pl.ds(lane, LANES)]
        mask = low_lanes(real.shape)
        first = jnp.where(mask, real, swap_halves(imag))
        second = jnp.where(mask, swap_halves(real), imag)
        chunk_refs[2 * pair][...] = jnp.where(side == 0, first, second)
        chunk_refs[2 * pair + 1][...] = jnp.where(side == 0, second, first)


COS1, COS2 = math.cos(2.0 * math.pi / 5), math.cos(4.0 * math.pi / 5)
SIN1, SIN2 = math.sin(2.0 * math.pi / 5), math.sin(4.0 * math.pi / 5)


def five_point(real, imag, sign):
    sum_r1, sum_i1 = real[1] + real[4], imag[1] + imag[4]
    sum_r2, sum_i2 = real[2] + real[3], imag[2] + imag[3]
    dif_r1, dif_i1 = real[1] - real[4], imag[1] - imag[4]
    dif_r2, dif_i2 = real[2] - real[3], imag[2] - imag[3]
    out_r0, out_i0 = real[0] + sum_r1 + sum_r2, imag[0] + sum_i1 + sum_i2
    even_r1 = real[0] + COS1 * sum_r1 + COS2 * sum_r2
    even_i1 = imag[0] + COS1 * sum_i1 + COS2 * sum_i2
    even_r2 = real[0] + COS2 * sum_r1 + COS1 * sum_r2
    even_i2 = imag[0] + COS2 * sum_i1 + COS1 * sum_i2
    odd_r1 = (sign * SIN1) * dif_r1 + (sign * SIN2) * dif_r2
    odd_i1 = (sign * SIN1) * dif_i1 + (sign * SIN2) * dif_i2
    odd_r2 = (sign * SIN2) * dif_r1 - (sign * SIN1) * dif_r2
    odd_i2 = (sign * SIN2) * dif_i1 - (sign * SIN1) * dif_i2
    return (
        [out_r0, even_r1 - odd_i1, even_r2 - odd_i2, even_r2 + odd_i2, even_r1 + odd_i1],
        [out_i0, even_i1 + odd_r1, even_i2 + odd_r2, even_i2 - odd_r2, even_i1 - odd_r1],
    )


def main_kernel(peers, inner, start_ref, stop_ref, matrix_ref, twist_ref, *refs):
    own_refs, sec_refs = refs[:peers], refs[peers : 2 * peers]
    out_refs = refs[2 * peers : 3 * peers]
    real_ref, imag_ref, mid_ref, high_ref, low_ref, sum_ref = refs[3 * peers :]
    me = lax.axis_index("line")
    date = lax.axis_index("date")
    chunk_lines = own_refs[0].shape[0]
    lines_all = peers * chunk_lines
    for r in range(peers):
        base = pl.multiple_of(jnp.bitwise_xor(me, r) * chunk_lines, 8)
        own, sec = own_refs[r][...], sec_refs[r][...]
        mask = low_lanes(own.shape)
        real_ref[pl.ds(base, chunk_lines), :] = jnp.where(mask, own, swap_halves(sec))
        imag_ref[pl.ds(base, chunk_lines), :] = jnp.where(mask, swap_halves(own), sec)

    high_table, low_table = matrix_ref[0], matrix_ref[1]

    def transform(high, low):
        return (
            jnp.dot(high_table, high, preferred_element_type=jnp.float32)
            + jnp.dot(high_table, low, preferred_element_type=jnp.float32)
            + jnp.dot(low_table, high, preferred_element_type=jnp.float32)
        )

    for l in range(LOOKS):
        real_high, real_low = split_pair(real_ref[pl.ds(l, inner, stride=LOOKS), :])
        imag_high, imag_low = split_pair(imag_ref[pl.ds(l, inner, stride=LOOKS), :])
        high = jnp.concatenate(
            [
                jnp.concatenate([real_high, imag_high], axis=1),
                jnp.concatenate([imag_high, -real_high], axis=1),
            ],
            axis=0,
        )
        low = jnp.concatenate(
            [
                jnp.concatenate([real_low, imag_low], axis=1),
                jnp.concatenate([imag_low, -real_low], axis=1),
            ],
            axis=0,
        )
        mid_ref[l] = transform(high, low)

    start, stop = start_ref[date], stop_ref[date]
    rows = 16

    def spectral(step, carry):
        row = pl.multiple_of(step * rows, rows)
        span = pl.ds(row, rows)
        real = [mid_ref[l, span, :LANES] for l in range(LOOKS)]
        imag = [mid_ref[l, span, LANES:] for l in range(LOOKS)]
        turn = [(twist_ref[l, 0, span, :], twist_ref[l, 1, span, :]) for l in range(LOOKS - 1)]
        for l in range(1, LOOKS):
            c, s = turn[l - 1]
            real[l], imag[l] = real[l] * c + imag[l] * s, imag[l] * c - real[l] * s
        real, imag = five_point(real, imag, -1.0)
        first = lax.broadcasted_iota(jnp.int32, (rows, LANES), 0) + row
        for m in range(LOOKS):
            bin_index = first + m * inner
            keep = (bin_index >= start) & (bin_index < stop)
            weight = jnp.where(keep, 1.0 / lines_all, 0.0)
            real[m], imag[m] = real[m] * weight, imag[m] * weight
        real, imag = five_point(real, imag, 1.0)
        for l in range(1, LOOKS):
            c, s = turn[l - 1]
            real[l], imag[l] = real[l] * c - imag[l] * s, imag[l] * c + real[l] * s
        span_below = pl.ds(pl.multiple_of(row + inner, rows), rows)
        for l in range(LOOKS):
            real_high, real_low = split_pair(real[l])
            imag_high, imag_low = split_pair(imag[l])
            high_ref[l, span, :LANES] = real_high
            high_ref[l, span, LANES:] = imag_high
            high_ref[l, span_below, :LANES] = -imag_high
            high_ref[l, span_below, LANES:] = real_high
            low_ref[l, span, :LANES] = real_low
            low_ref[l, span, LANES:] = imag_low
            low_ref[l, span_below, :LANES] = -imag_low
            low_ref[l, span_below, LANES:] = real_low
        return carry

    lax.fori_loop(0, inner // rows, spectral, 0)

    total = None
    for l in range(LOOKS):
        signal = transform(high_ref[l], low_ref[l])
        real, imag = signal[:, :LANES], signal[:, LANES:]
        real_other, imag_other = swap_halves(real), swap_halves(imag)
        product = jnp.where(
            low_lanes(real.shape),
            real * real_other + imag * imag_other,
            real * imag_other - imag * real_other,
        )
        total = product if total is None else total + product
    sum_ref[...] = total * (1.0 / LOOKS)
    out_lines = inner // peers
    for r in range(peers):
        base = pl.multiple_of(jnp.bitwise_xor(me, r) * out_lines, 8)
        out_refs[r][...] = sum_ref[pl.ds(base, out_lines), :]


def unpack_kernel(peers, *refs):
    chunk_refs, out_ref = refs[:peers], refs[peers]
    me = lax.axis_index("line")
    side = me % 2
    for pair in range(peers // 2):
        block = jnp.bitwise_xor(me // 2, pair)
        lane = pl.multiple_of(block * LANES, LANES)
        even, odd = chunk_refs[2 * pair][...], chunk_refs[2 * pair + 1][...]
        first = jnp.where(side == 0, even, odd)
        second = jnp.where(side == 0, odd, even)
        mask = low_lanes(first.shape)
        out_ref[0, :, pl.ds(lane, LANES)] = jnp.where(mask, first, swap_halves(second))
        out_ref[1, :, pl.ds(lane, LANES)] = jnp.where(mask, swap_halves(first), second)


def packed_step(slc, band_start, band_stop):
    peers = lax.axis_size("line")
    chunk_lines = slc.shape[3]
    inner = peers * chunk_lines // LOOKS
    out_lines = inner // peers
    f32 = jnp.float32
    vmem = pl.BlockSpec(memory_space=pltpu.VMEM)
    smem = pl.BlockSpec(memory_space=pltpu.SMEM)
    chunk = jax.ShapeDtypeStruct((chunk_lines, LANES), f32)
    image = jnp.transpose(slc[0], (0, 2, 1))
    packed = pl.pallas_call(
        functools.partial(pack_kernel, peers),
        out_shape=[chunk] * peers,
        in_specs=[vmem],
        out_specs=[vmem] * peers,
        compiler_params=pltpu.CompilerParams(vmem_limit_bytes=8 * MIB),
        name="pack",
    )(image)

    def exchange(values, r):
        return lax.ppermute(values, "line", [(i, i ^ r) for i in range(peers)])

    def forward(values):
        return shifted(values, "date", -1)

    own = [values if r == 0 else exchange(values, r) for r, values in enumerate(packed)]
    sec = [forward(values) for values in own]
    matrix, twist = host_tables(inner)
    looked = pl.pallas_call(
        functools.partial(main_kernel, peers, inner),
        out_shape=[jax.ShapeDtypeStruct((out_lines, LANES), f32)] * peers,
        in_specs=[smem, smem, vmem, vmem] + [vmem] * (2 * peers),
        out_specs=[vmem] * peers,
        scratch_shapes=[
            pltpu.VMEM((peers * chunk_lines, LANES), f32),
            pltpu.VMEM((peers * chunk_lines, LANES), f32),
            pltpu.VMEM((LOOKS, inner, 2 * LANES), f32),
            pltpu.VMEM((LOOKS, 2 * inner, 2 * LANES), jnp.bfloat16),
            pltpu.VMEM((LOOKS, 2 * inner, 2 * LANES), jnp.bfloat16),
            pltpu.VMEM((inner, LANES), f32),
        ],
        compiler_params=pltpu.CompilerParams(vmem_limit_bytes=24 * MIB),
        name="interfere",
    )(band_start, band_stop, jnp.asarray(matrix), jnp.asarray(twist), *own, *sec)
    looked = [values if r == 0 else exchange(values, r) for r, values in enumerate(looked)]
    result = pl.pallas_call(
        functools.partial(unpack_kernel, peers),
        out_shape=jax.ShapeDtypeStruct((2, out_lines, slc.shape[2]), f32),
        in_specs=[vmem] * peers,
        out_specs=vmem,
        compiler_params=pltpu.CompilerParams(vmem_limit_bytes=8 * MIB),
        name="unpack",
    )(*looked)
    return jnp.transpose(result, (0, 2, 1))[None]


def packs(mesh, slc):
    peers = mesh.shape["line"]
    columns = slc.shape[2] // mesh.shape["stack"] // peers
    chunk_lines = slc.shape[3] // peers
    inner = slc.shape[3] // LOOKS
    return (
        peers > 1
        and peers & (peers - 1) == 0
        and columns == HALF
        and chunk_lines % 8 == 0
        and inner % (8 * peers) == 0
        and inner % LANES == 0
        and inner <= 4 * LANES
    )


def solution(mesh):
    specs = dict(
        mesh=mesh,
        in_specs=(P("date", None, "stack", "line"), P(), P()),
        out_specs=P("date", None, "stack", "line"),
        check_vma=False,
    )

    def whole(slc, band_start, band_stop):
        if not packs(mesh, slc):
            return jax.shard_map(general_shards, **specs)(slc, band_start, band_stop)
        step = jax.shard_map(packed_step, **specs)
        return step(slc, band_start, band_stop)

    return whole
```

```python
import functools
import math

import jax
import jax.numpy as jnp
import numpy as np
from jax import lax
from jax.experimental import pallas as pl
from jax.experimental.pallas import tpu as pltpu
from jax.sharding import PartitionSpec as P


LOOKS = 5
TAPS = 2 * LOOKS
LANES = 128
MIB = 1 << 20
HALF = LANES // 2


HIGHEST_PRECISION = lax.Precision.HIGHEST


def shifted(shard, axis, by):
    size = lax.axis_size(axis)
    return lax.ppermute(shard, axis, [(i, (i + by) % size) for i in range(size)])


def phase_table(count, sign_value):
    index_row = jnp.arange(count, dtype=jnp.int32)
    wrapped = index_row[:, None] * index_row[None, :] % count
    angle_all = 2.0 * math.pi / count * wrapped.astype(jnp.float32)
    return (jnp.cos(angle_all), sign_value * jnp.sin(angle_all))


def twiddle_table(outer, inner, sign_value):
    outer_row = jnp.arange(outer, dtype=jnp.int32)
    inner_row = jnp.arange(inner, dtype=jnp.int32)
    wrapped = outer_row[:, None] * inner_row[None, :] % (outer * inner)
    angle_all = 2.0 * math.pi / (outer * inner) * wrapped.astype(jnp.float32)
    return (jnp.cos(angle_all), sign_value * jnp.sin(angle_all))


def left_product(table_real, table_imag, data_real, data_imag):

    def single(table, data):
        return jnp.einsum("ka,cab->ckb", table, data, precision=HIGHEST_PRECISION)

    return (
        single(table_real, data_real) - single(table_imag, data_imag),
        single(table_real, data_imag) + single(table_imag, data_real),
    )


def right_product(data_real, data_imag, table_real, table_imag):

    def single(data, table):
        return jnp.einsum("ckb,bm->ckm", data, table, precision=HIGHEST_PRECISION)

    return (
        single(data_real, table_real) - single(data_imag, table_imag),
        single(data_imag, table_real) + single(data_real, table_imag),
    )


def forward_dft(data_real, data_imag):
    outer = data_real.shape[1]
    inner = data_real.shape[2]
    outer_real, outer_imag = phase_table(outer, -1.0)
    first_real, first_imag = left_product(outer_real, outer_imag, data_real, data_imag)
    twist_real, twist_imag = twiddle_table(outer, inner, -1.0)
    turned_real = first_real * twist_real - first_imag * twist_imag
    turned_imag = first_real * twist_imag + first_imag * twist_real
    inner_real, inner_imag = phase_table(inner, -1.0)
    return right_product(turned_real, turned_imag, inner_real, inner_imag)


def inverse_dft(data_real, data_imag):
    outer = data_real.shape[1]
    inner = data_real.shape[2]
    inner_real, inner_imag = phase_table(inner, 1.0)
    first_real, first_imag = right_product(data_real, data_imag, inner_real, inner_imag)
    twist_real, twist_imag = twiddle_table(outer, inner, 1.0)
    turned_real = first_real * twist_real - first_imag * twist_imag
    turned_imag = first_real * twist_imag + first_imag * twist_real
    outer_real, outer_imag = phase_table(outer, 1.0)
    result_real, result_imag = left_product(outer_real, outer_imag, turned_real, turned_imag)
    scale = 1.0 / (outer * inner)
    return (result_real * scale, result_imag * scale)


def conj_product(ref_real, ref_imag, sec_real, sec_imag):
    return (ref_real * sec_real + ref_imag * sec_imag, ref_imag * sec_real - ref_real * sec_imag)


def look_mean(values):
    return values.reshape(values.shape[0], values.shape[1] // LOOKS, LOOKS).sum(axis=-1) * (
        1.0 / LOOKS
    )


def general_shards(slc, band_start, band_stop):
    own_image = slc[0]
    line_lines = own_image.shape[2]
    turned = lax.all_to_all(own_image, "line", split_axis=1, concat_axis=2, tiled=True)
    columns = turned.shape[1]
    outer = lax.axis_size("line")
    lines_all = outer * line_lines
    blocks = turned.reshape(2, columns, outer, line_lines)
    spec_real, spec_imag = forward_dft(blocks[0], blocks[1])
    spectrum = jnp.stack([spec_real, spec_imag], axis=0)
    date_index = lax.axis_index("date")
    my_start = lax.dynamic_slice_in_dim(band_start, date_index, 1)[0]
    my_end = lax.dynamic_slice_in_dim(band_stop, date_index, 1)[0]
    bin_index = (
        jnp.arange(outer, dtype=jnp.int32)[:, None]
        + outer * jnp.arange(line_lines, dtype=jnp.int32)[None, :]
    )
    keep_mask = ((bin_index >= my_start) & (bin_index < my_end)).astype(jnp.float32)
    partner = shifted(spectrum, "date", -1)
    ref_spec = spectrum * keep_mask
    sec_spec = partner * keep_mask
    both_real, both_imag = inverse_dft(
        jnp.concatenate([ref_spec[0], sec_spec[0]], axis=0),
        jnp.concatenate([ref_spec[1], sec_spec[1]], axis=0),
    )
    ref_real = both_real[:columns].reshape(columns, lines_all)
    ref_imag = both_imag[:columns].reshape(columns, lines_all)
    sec_real = both_real[columns:].reshape(columns, lines_all)
    sec_imag = both_imag[columns:].reshape(columns, lines_all)
    prod_real, prod_imag = conj_product(ref_real, ref_imag, sec_real, sec_imag)
    looked = jnp.stack([look_mean(prod_real), look_mean(prod_imag)], axis=0)
    result = lax.all_to_all(looked, "line", split_axis=2, concat_axis=1, tiled=True)
    return result[None]


def split_pair(values):
    high = values.astype(jnp.bfloat16)
    low = (values - high.astype(jnp.float32)).astype(jnp.bfloat16)
    return high, low


@functools.lru_cache(maxsize=None)
def host_tables(inner, chunk_lines, last):
    lines_all = TAPS * inner
    bins, steps, taps = np.arange(inner), np.arange(inner), np.arange(TAPS)
    turns = bins[None, :, None] * (TAPS * steps[None, None, :] + taps[:, None, None]) % lines_all
    angle = 2.0 * np.pi / lines_all * turns
    cos, sin = np.cos(angle), np.sin(angle)

    def halves(table):
        high = table.astype(jnp.bfloat16)
        low = (table - high.astype(np.float64)).astype(jnp.bfloat16)
        return high, low

    ahead = halves(np.concatenate([cos, sin], axis=2))
    swapped = [np.swapaxes(table, 1, 2) for table in (cos, -sin)]
    back = halves(np.concatenate(swapped, axis=2))
    few = chunk_lines // TAPS
    part = slice(last * few, (last + 1) * few)
    high, low = halves(np.concatenate([cos[:, :, part], sin[:, :, part]], axis=2))
    late = np.concatenate([high, high, low], axis=2)
    late = np.pad(late, ((0, 0), (0, 0), (0, -late.shape[2] % (2 * LANES))))
    return np.stack(ahead), np.stack(back), late


def low_lanes(shape):
    return lax.broadcasted_iota(jnp.int32, shape, len(shape) - 1) < HALF


def swap_halves(values):
    return pltpu.roll(values, HALF, values.ndim - 1)


def pack_kernel(peers, image_ref, *chunk_refs):
    me = lax.axis_index("line")
    side = me % 2
    for pair in range(peers // 2):
        block = jnp.bitwise_xor(me // 2, pair)
        lane = pl.multiple_of(block * LANES, LANES)
        real = image_ref[0, :, pl.ds(lane, LANES)]
        imag = image_ref[1, :, pl.ds(lane, LANES)]
        mask = low_lanes(real.shape)
        first = jnp.where(mask, real, swap_halves(imag))
        second = jnp.where(mask, swap_halves(real), imag)
        chunk_refs[2 * pair][...] = jnp.where(side == 0, first, second)
        chunk_refs[2 * pair + 1][...] = jnp.where(side == 0, second, first)


COS1, COS2 = math.cos(2.0 * math.pi / 5), math.cos(4.0 * math.pi / 5)
SIN1, SIN2 = math.sin(2.0 * math.pi / 5), math.sin(4.0 * math.pi / 5)


def five_point(real, imag, sign):
    sum_r1, sum_i1 = real[1] + real[4], imag[1] + imag[4]
    sum_r2, sum_i2 = real[2] + real[3], imag[2] + imag[3]
    dif_r1, dif_i1 = real[1] - real[4], imag[1] - imag[4]
    dif_r2, dif_i2 = real[2] - real[3], imag[2] - imag[3]
    out_r0, out_i0 = real[0] + sum_r1 + sum_r2, imag[0] + sum_i1 + sum_i2
    even_r1 = real[0] + COS1 * sum_r1 + COS2 * sum_r2
    even_i1 = imag[0] + COS1 * sum_i1 + COS2 * sum_i2
    even_r2 = real[0] + COS2 * sum_r1 + COS1 * sum_r2
    even_i2 = imag[0] + COS2 * sum_i1 + COS1 * sum_i2
    odd_r1 = (sign * SIN1) * dif_r1 + (sign * SIN2) * dif_r2
    odd_i1 = (sign * SIN1) * dif_i1 + (sign * SIN2) * dif_i2
    odd_r2 = (sign * SIN2) * dif_r1 - (sign * SIN1) * dif_r2
    odd_i2 = (sign * SIN2) * dif_i1 - (sign * SIN1) * dif_i2
    return (
        [out_r0, even_r1 - odd_i1, even_r2 - odd_i2, even_r2 + odd_i2, even_r1 + odd_i1],
        [out_i0, even_i1 + odd_r1, even_i2 + odd_r2, even_i2 - odd_r2, even_i1 - odd_r1],
    )


def ten_point(real, imag, sign):
    first = [2 * b % TAPS for b in range(LOOKS)]
    other = [(LOOKS + 2 * b) % TAPS for b in range(LOOKS)]
    out_real, out_imag = [None] * TAPS, [None] * TAPS
    for c in range(2):
        join = (lambda x, y: x - y) if c else (lambda x, y: x + y)
        part_real = [join(real[i], real[j]) for i, j in zip(first, other)]
        part_imag = [join(imag[i], imag[j]) for i, j in zip(first, other)]
        part_real, part_imag = five_point(part_real, part_imag, sign)
        for m in range(TAPS):
            if m % 2 == c:
                out_real[m], out_imag[m] = part_real[m % LOOKS], part_imag[m % LOOKS]
    return out_real, out_imag


def quadrants(real, imag):
    return jnp.concatenate(
        [jnp.concatenate([real, imag], axis=1), jnp.concatenate([imag, -real], axis=1)], axis=0
    )


def block_of(me, r, peers):
    return (jnp.bitwise_xor(me, r) - me) % peers


def product(table, data):
    return jnp.dot(table, data, preferred_element_type=jnp.float32)


def transform(table_ref, tap, real, imag):
    real_high, real_low = split_pair(real)
    imag_high, imag_low = split_pair(imag)
    high, low = quadrants(real_high, imag_high), quadrants(real_low, imag_low)
    table_high, table_low = table_ref[0, tap], table_ref[1, tap]
    return product(table_high, high) + product(table_low, high) + product(table_high, low)


def tables_kernel(count, *refs):
    for source, target in zip(refs[:count], refs[count:]):
        target[...] = source[...]


def early_kernel(peers, last, table_ref, *refs):
    own_refs, sec_refs = refs[:peers], list(refs[peers : 2 * peers - 1])
    out_ref, real_ref, imag_ref = refs[2 * peers - 1 :]
    sec_refs.insert(last, None)
    me = lax.axis_index("line")
    chunk_lines = own_refs[0].shape[0]
    inner = peers * chunk_lines // TAPS
    for r in range(peers):
        base = pl.multiple_of(block_of(me, r, peers) * chunk_lines, 8)
        own = own_refs[r][...]
        mask = low_lanes(own.shape)
        if r == last:
            real, imag = jnp.where(mask, own, 0.0), jnp.where(mask, swap_halves(own), 0.0)
        else:
            sec = sec_refs[r][...]
            real, imag = jnp.where(mask, own, swap_halves(sec)), jnp.where(mask, swap_halves(own), sec)
        real_ref[pl.ds(base, chunk_lines), :] = real
        imag_ref[pl.ds(base, chunk_lines), :] = imag
    for l in range(TAPS):
        span = pl.ds(l, inner, stride=TAPS)
        out_ref[l] = transform(table_ref, l, real_ref[span, :], imag_ref[span, :])


def late_kernel(
    peers, start_ref, stop_ref, late_ref, back_ref, mid_ref, sec_ref, *refs
):
    out_refs = refs[:peers]
    real_ref, imag_ref, sum_ref = refs[peers:]
    me = lax.axis_index("line")
    date = lax.axis_index("date")
    chunk_lines = sec_ref.shape[0]
    inner = peers * chunk_lines // TAPS
    few = chunk_lines // TAPS
    sec = sec_ref[...]
    mask = low_lanes(sec.shape)
    real_ref[0:chunk_lines, :] = jnp.where(mask, 0.0, swap_halves(sec))
    imag_ref[0:chunk_lines, :] = jnp.where(mask, 0.0, sec)
    for l in range(TAPS):
        span = pl.ds(l, few, stride=TAPS)
        real_high, real_low = split_pair(real_ref[span, :])
        imag_high, imag_low = split_pair(imag_ref[span, :])
        high, low = quadrants(real_high, imag_high), quadrants(real_low, imag_low)
        rest = jnp.zeros((late_ref.shape[2] - 6 * few, 2 * LANES), jnp.bfloat16)
        mid_ref[l] += product(late_ref[l], jnp.concatenate([high, low, high, rest], axis=0))

    start, stop = start_ref[date], stop_ref[date]
    width = stop - start
    rows = 8

    def spectral(step, carry):
        row = pl.multiple_of(step * rows, rows)
        span = pl.ds(row, rows)
        real = [mid_ref[l, span, :LANES] for l in range(TAPS)]
        imag = [mid_ref[l, span, LANES:] for l in range(TAPS)]
        real, imag = ten_point(real, imag, -1.0)
        first = lax.broadcasted_iota(jnp.int32, (rows, LANES), 0) + (row - start)
        for m in range(TAPS):
            offset = first + m * inner
            keep = (offset >= 0) & (offset < width)
            real[m], imag[m] = jnp.where(keep, real[m], 0.0), jnp.where(keep, imag[m], 0.0)
        real, imag = ten_point(real, imag, 1.0)
        for l in range(TAPS):
            mid_ref[l, span, :LANES] = real[l]
            mid_ref[l, span, LANES:] = imag[l]
        return carry

    lax.fori_loop(0, inner // rows, spectral, 0)

    lines_all = peers * chunk_lines
    scale = 1.0 / (lines_all * lines_all * LOOKS)
    for half in range(2):
        total = None
        for l in range(half * LOOKS, (half + 1) * LOOKS):
            signal = transform(back_ref, l, mid_ref[l, :, :LANES], mid_ref[l, :, LANES:])
            real, imag = signal[:, :LANES], signal[:, LANES:]
            real_other, imag_other = swap_halves(real), swap_halves(imag)
            value = jnp.where(
                low_lanes(real.shape),
                real * real_other + imag * imag_other,
                real * imag_other - imag * real_other,
            )
            total = value if total is None else total + value
        sum_ref[pl.ds(half, inner, stride=2), :] = total * scale
    out_lines = 2 * inner // peers
    for r in range(peers):
        base = pl.multiple_of(block_of(me, r, peers) * out_lines, 8)
        out_refs[r][...] = sum_ref[pl.ds(base, out_lines), :]


def unpack_kernel(peers, *refs):
    chunk_refs, out_ref = refs[:peers], refs[peers]
    me = lax.axis_index("line")
    side = me % 2
    for pair in range(peers // 2):
        block = jnp.bitwise_xor(me // 2, pair)
        lane = pl.multiple_of(block * LANES, LANES)
        even, odd = chunk_refs[2 * pair][...], chunk_refs[2 * pair + 1][...]
        first = jnp.where(side == 0, even, odd)
        second = jnp.where(side == 0, odd, even)
        mask = low_lanes(first.shape)
        out_ref[0, :, pl.ds(lane, LANES)] = jnp.where(mask, first, swap_halves(second))
        out_ref[1, :, pl.ds(lane, LANES)] = jnp.where(mask, swap_halves(first), second)


def packed_step(slc, band_start, band_stop):
    peers = lax.axis_size("line")
    chunk_lines = slc.shape[3]
    inner = peers * chunk_lines // TAPS
    out_lines = 2 * inner // peers
    f32 = jnp.float32
    vmem = pl.BlockSpec(memory_space=pltpu.VMEM)
    smem = pl.BlockSpec(memory_space=pltpu.SMEM)
    chunk = jax.ShapeDtypeStruct((chunk_lines, LANES), f32)
    image = jnp.transpose(slc[0], (0, 2, 1))
    packed = pl.pallas_call(
        functools.partial(pack_kernel, peers),
        out_shape=[chunk] * peers,
        in_specs=[vmem],
        out_specs=[vmem] * peers,
        compiler_params=pltpu.CompilerParams(vmem_limit_bytes=8 * MIB),
        name="pack",
    )(image)

    def exchange(values, r):
        return lax.ppermute(values, "line", [(i, i ^ r) for i in range(peers)])

    def forward(values):
        return shifted(values, "date", -1)

    own = [values if r == 0 else exchange(values, r) for r, values in enumerate(packed)]
    sec = [forward(values) for values in own]
    last = peers // 2
    tables = [jnp.asarray(table) for table in host_tables(inner, chunk_lines, last)]
    ahead, back, late = pl.pallas_call(
        functools.partial(tables_kernel, len(tables)),
        out_shape=[jax.ShapeDtypeStruct(table.shape, table.dtype) for table in tables],
        in_specs=[vmem] * len(tables),
        out_specs=[vmem] * len(tables),
        compiler_params=pltpu.CompilerParams(vmem_limit_bytes=16 * MIB),
        name="tables",
    )(*tables)
    planes = pltpu.VMEM((peers * chunk_lines, LANES), f32)
    middle = pl.pallas_call(
        functools.partial(early_kernel, peers, last),
        out_shape=jax.ShapeDtypeStruct((TAPS, inner, 2 * LANES), f32),
        in_specs=[vmem] * (2 * peers),
        out_specs=vmem,
        scratch_shapes=[planes, planes],
        compiler_params=pltpu.CompilerParams(vmem_limit_bytes=16 * MIB),
        name="early",
    )(ahead, *own, *(values for r, values in enumerate(sec) if r != last))
    part = pltpu.VMEM((chunk_lines, LANES), f32)
    looked = pl.pallas_call(
        functools.partial(late_kernel, peers),
        out_shape=[jax.ShapeDtypeStruct((out_lines, LANES), f32)] * peers,
        in_specs=[smem, smem] + [vmem] * 4,
        out_specs=[vmem] * peers,
        scratch_shapes=[part, part, pltpu.VMEM((2 * inner, LANES), f32)],
        compiler_params=pltpu.CompilerParams(vmem_limit_bytes=16 * MIB),
        name="late",
    )(band_start, band_stop, late, back, middle, sec[last])
    looked = [values if r == 0 else exchange(values, r) for r, values in enumerate(looked)]
    result = pl.pallas_call(
        functools.partial(unpack_kernel, peers),
        out_shape=jax.ShapeDtypeStruct((2, out_lines, slc.shape[2]), f32),
        in_specs=[vmem] * peers,
        out_specs=vmem,
        compiler_params=pltpu.CompilerParams(vmem_limit_bytes=8 * MIB),
        name="unpack",
    )(*looked)
    return jnp.transpose(result, (0, 2, 1))[None]


def packs(mesh, slc):
    peers = mesh.shape["line"]
    columns = slc.shape[2] // mesh.shape["stack"] // peers
    chunk_lines = slc.shape[3] // peers
    inner = slc.shape[3] // TAPS
    return (
        columns == HALF
        and peers == 4
        and chunk_lines % (16 * TAPS) == 0
        and inner % LANES == 0
        and inner <= 4 * LANES
    )


def solution(mesh):
    specs = dict(
        mesh=mesh,
        in_specs=(P("date", None, "stack", "line"), P(), P()),
        out_specs=P("date", None, "stack", "line"),
        check_vma=False,
    )

    def whole(slc, band_start, band_stop):
        if not packs(mesh, slc):
            return jax.shard_map(general_shards, **specs)(slc, band_start, band_stop)
        step = jax.shard_map(packed_step, **specs)
        return step(slc, band_start, band_stop)

    return whole
```

```python
import functools
import math

import jax
import jax.numpy as jnp
import numpy as np
from jax import lax
from jax.experimental import pallas as pl
from jax.experimental.pallas import tpu as pltpu
from jax.sharding import PartitionSpec as P


LOOKS = 5
TAPS = 2 * LOOKS
EXCHANGE = ((3, 2, 1, 0), (1, 0, 3, 2), (2, 3, 0, 1))
RETURN = ((2, 3, 0, 1), (3, 2, 1, 0), (1, 0, 3, 2))
LANES = 128
MIB = 1 << 20
HALF = LANES // 2


HIGHEST_PRECISION = lax.Precision.HIGHEST


def shifted(shard, axis, by):
    size = lax.axis_size(axis)
    return lax.ppermute(shard, axis, [(i, (i + by) % size) for i in range(size)])


def phase_table(count, sign_value):
    index_row = jnp.arange(count, dtype=jnp.int32)
    wrapped = index_row[:, None] * index_row[None, :] % count
    angle_all = 2.0 * math.pi / count * wrapped.astype(jnp.float32)
    return (jnp.cos(angle_all), sign_value * jnp.sin(angle_all))


def twiddle_table(outer, inner, sign_value):
    outer_row = jnp.arange(outer, dtype=jnp.int32)
    inner_row = jnp.arange(inner, dtype=jnp.int32)
    wrapped = outer_row[:, None] * inner_row[None, :] % (outer * inner)
    angle_all = 2.0 * math.pi / (outer * inner) * wrapped.astype(jnp.float32)
    return (jnp.cos(angle_all), sign_value * jnp.sin(angle_all))


def left_product(table_real, table_imag, data_real, data_imag):

    def single(table, data):
        return jnp.einsum("ka,cab->ckb", table, data, precision=HIGHEST_PRECISION)

    return (
        single(table_real, data_real) - single(table_imag, data_imag),
        single(table_real, data_imag) + single(table_imag, data_real),
    )


def right_product(data_real, data_imag, table_real, table_imag):

    def single(data, table):
        return jnp.einsum("ckb,bm->ckm", data, table, precision=HIGHEST_PRECISION)

    return (
        single(data_real, table_real) - single(data_imag, table_imag),
        single(data_imag, table_real) + single(data_real, table_imag),
    )


def forward_dft(data_real, data_imag):
    outer = data_real.shape[1]
    inner = data_real.shape[2]
    outer_real, outer_imag = phase_table(outer, -1.0)
    first_real, first_imag = left_product(outer_real, outer_imag, data_real, data_imag)
    twist_real, twist_imag = twiddle_table(outer, inner, -1.0)
    turned_real = first_real * twist_real - first_imag * twist_imag
    turned_imag = first_real * twist_imag + first_imag * twist_real
    inner_real, inner_imag = phase_table(inner, -1.0)
    return right_product(turned_real, turned_imag, inner_real, inner_imag)


def inverse_dft(data_real, data_imag):
    outer = data_real.shape[1]
    inner = data_real.shape[2]
    inner_real, inner_imag = phase_table(inner, 1.0)
    first_real, first_imag = right_product(data_real, data_imag, inner_real, inner_imag)
    twist_real, twist_imag = twiddle_table(outer, inner, 1.0)
    turned_real = first_real * twist_real - first_imag * twist_imag
    turned_imag = first_real * twist_imag + first_imag * twist_real
    outer_real, outer_imag = phase_table(outer, 1.0)
    result_real, result_imag = left_product(outer_real, outer_imag, turned_real, turned_imag)
    scale = 1.0 / (outer * inner)
    return (result_real * scale, result_imag * scale)


def conj_product(ref_real, ref_imag, sec_real, sec_imag):
    return (ref_real * sec_real + ref_imag * sec_imag, ref_imag * sec_real - ref_real * sec_imag)


def look_mean(values):
    return values.reshape(values.shape[0], values.shape[1] // LOOKS, LOOKS).sum(axis=-1) * (
        1.0 / LOOKS
    )


def general_shards(slc, band_start, band_stop):
    own_image = slc[0]
    line_lines = own_image.shape[2]
    turned = lax.all_to_all(own_image, "line", split_axis=1, concat_axis=2, tiled=True)
    columns = turned.shape[1]
    outer = lax.axis_size("line")
    lines_all = outer * line_lines
    blocks = turned.reshape(2, columns, outer, line_lines)
    spec_real, spec_imag = forward_dft(blocks[0], blocks[1])
    spectrum = jnp.stack([spec_real, spec_imag], axis=0)
    date_index = lax.axis_index("date")
    my_start = lax.dynamic_slice_in_dim(band_start, date_index, 1)[0]
    my_end = lax.dynamic_slice_in_dim(band_stop, date_index, 1)[0]
    bin_index = (
        jnp.arange(outer, dtype=jnp.int32)[:, None]
        + outer * jnp.arange(line_lines, dtype=jnp.int32)[None, :]
    )
    keep_mask = ((bin_index >= my_start) & (bin_index < my_end)).astype(jnp.float32)
    partner = shifted(spectrum, "date", -1)
    ref_spec = spectrum * keep_mask
    sec_spec = partner * keep_mask
    both_real, both_imag = inverse_dft(
        jnp.concatenate([ref_spec[0], sec_spec[0]], axis=0),
        jnp.concatenate([ref_spec[1], sec_spec[1]], axis=0),
    )
    ref_real = both_real[:columns].reshape(columns, lines_all)
    ref_imag = both_imag[:columns].reshape(columns, lines_all)
    sec_real = both_real[columns:].reshape(columns, lines_all)
    sec_imag = both_imag[columns:].reshape(columns, lines_all)
    prod_real, prod_imag = conj_product(ref_real, ref_imag, sec_real, sec_imag)
    looked = jnp.stack([look_mean(prod_real), look_mean(prod_imag)], axis=0)
    result = lax.all_to_all(looked, "line", split_axis=2, concat_axis=1, tiled=True)
    return result[None]


def split_pair(values):
    high = values.astype(jnp.bfloat16)
    low = (values - high.astype(jnp.float32)).astype(jnp.bfloat16)
    return high, low


@functools.lru_cache(maxsize=None)
def host_tables(inner, first_step, few):
    lines_all = TAPS * inner
    bins, steps, taps = np.arange(inner), np.arange(inner), np.arange(TAPS)
    turns = bins[None, :, None] * (TAPS * steps[None, None, :] + taps[:, None, None]) % lines_all
    angle = 2.0 * np.pi / lines_all * turns
    cos, sin = np.cos(angle), np.sin(angle)

    def halves(table):
        high = table.astype(jnp.bfloat16)
        low = (table - high.astype(np.float64)).astype(jnp.bfloat16)
        return high, low

    ahead = halves(np.concatenate([cos, sin], axis=2))
    swapped = [np.swapaxes(table, 1, 2) for table in (cos, -sin)]
    back = halves(np.concatenate(swapped, axis=2))
    part = slice(first_step, first_step + few)
    high, low = halves(np.concatenate([cos[:, :, part], sin[:, :, part]], axis=2))
    late = np.concatenate([high, high, low], axis=2)
    late = np.pad(late, ((0, 0), (0, 0), (0, -late.shape[2] % LANES)))
    return np.stack(ahead), np.stack(back), late


def low_lanes(shape):
    return lax.broadcasted_iota(jnp.int32, shape, len(shape) - 1) < HALF


def swap_halves(values):
    return pltpu.roll(values, HALF, values.ndim - 1)


def turned(values):
    other = swap_halves(values)
    return jnp.where(low_lanes(values.shape), other, -other)


def entry(row, me):
    code = sum(value << (4 * place) for place, value in enumerate(row))
    return jnp.bitwise_and(jnp.right_shift(jnp.int32(code), 4 * me), 15)


def senders(row):
    return tuple(row.index(place) for place in range(len(row)))


def pack_kernel(image_ref, *chunk_refs):
    me = lax.axis_index("line")
    for row, chunk_ref in zip((None,) + EXCHANGE, chunk_refs):
        block = me if row is None else entry(row, me)
        lane = pl.multiple_of(block // 2 * LANES, LANES)
        side = block % 2
        stay = image_ref[side, :, pl.ds(lane, LANES)]
        move = image_ref[1 - side, :, pl.ds(lane, LANES)]
        half = lax.broadcasted_iota(jnp.int32, stay.shape, 1) // HALF
        chunk_ref[...] = jnp.where(half == side, stay, swap_halves(move))


COS1, COS2 = math.cos(2.0 * math.pi / 5), math.cos(4.0 * math.pi / 5)
SIN1, SIN2 = math.sin(2.0 * math.pi / 5), math.sin(4.0 * math.pi / 5)


def five_point(x, sign):
    unit = jnp.where(low_lanes(x[0].shape), sign, -sign)
    sin1, sin2 = SIN1 * unit, SIN2 * unit
    sum1, sum2 = x[1] + x[4], x[2] + x[3]
    dif1, dif2 = x[1] - x[4], x[2] - x[3]
    even1 = x[0] + COS1 * sum1 + COS2 * sum2
    even2 = x[0] + COS2 * sum1 + COS1 * sum2
    odd1 = swap_halves(sin1 * dif1 + sin2 * dif2)
    odd2 = swap_halves(sin2 * dif1 - sin1 * dif2)
    return [x[0] + sum1 + sum2, even1 + odd1, even2 + odd2, even2 - odd2, even1 - odd1]


def ten_point(x, sign):
    first = [x[2 * b % TAPS] for b in range(LOOKS)]
    other = [x[(LOOKS + 2 * b) % TAPS] for b in range(LOOKS)]
    even = five_point([p + q for p, q in zip(first, other)], sign)
    odd = five_point([p - q for p, q in zip(first, other)], sign)
    return [(odd if m % 2 else even)[m % LOOKS] for m in range(TAPS)]


def block_of(me, block, peers):
    return (block - entry(senders(EXCHANGE[-1]), me)) % peers


def product(table, data):
    return jnp.dot(table, data, preferred_element_type=jnp.float32)


def stacked(*values):
    return jnp.concatenate(values, axis=0)


def beside(*values):
    return jnp.concatenate(values, axis=1)


def spectral(mid_ref, weight_ref, back_ref):
    rows = 8

    def block(step, carry):
        span = pl.ds(pl.multiple_of(step * rows, rows), rows)
        x = ten_point([mid_ref[l, span, :] for l in range(TAPS)], -1.0)
        x = ten_point([x[m] * weight_ref[m, span, :] for m in range(TAPS)], 1.0)
        for l in range(TAPS):
            back_ref[l, span, :] = x[l]
        return carry

    lax.fori_loop(0, mid_ref.shape[1] // rows, block, 0, unroll=True)


def signal_of(mid_ref, back_ref, l):
    values = mid_ref[l]
    high, low = split_pair(stacked(values, turned(values)))
    both = beside(high, low)
    signal = product(back_ref[0, l], both) + product(back_ref[1, l], both)
    return signal[:, :LANES] + signal[:, LANES:]


def tables_kernel(count, *refs):
    for source, target in zip(refs[:count], refs[count:]):
        target[...] = source[...]


def early_kernel(peers, start_ref, stop_ref, ahead_ref, back_ref, *refs):
    own_refs, sec_refs = refs[:peers], refs[peers : 2 * peers - 1]
    mid_ref, weight_ref, same_ref, cross_ref = refs[2 * peers - 1 : 2 * peers + 3]
    own_ref, own_turned_ref, sec_ref, sec_turned_ref = refs[2 * peers + 3 : -2]
    own_mid_ref, own_back_ref = refs[-2:]
    me = lax.axis_index("line")
    date = lax.axis_index("date")
    lines = own_ref.shape[0] // peers
    inner = own_ref.shape[0] // TAPS
    for q in range(peers):
        block = entry(senders(EXCHANGE[q - 1]), me) if q else me
        span = pl.ds(pl.multiple_of(block_of(me, block, peers) * lines, 8), lines)
        own = own_refs[q][...]
        own_ref[span, :] = own
        own_turned_ref[span, :] = turned(own)
        if q == peers - 1:
            sec_ref[span, :] = jnp.zeros((lines, LANES), jnp.float32)
            sec_turned_ref[span, :] = jnp.zeros((lines, LANES), jnp.float32)
        else:
            sec = sec_refs[q][...]
            sec_ref[span, :] = sec
            sec_turned_ref[span, :] = turned(sec)
    for l in range(TAPS):
        span = pl.ds(l, inner, stride=TAPS)
        high, low = split_pair(
            stacked(
                beside(own_ref[span, :], sec_ref[span, :]),
                beside(own_turned_ref[span, :], sec_turned_ref[span, :]),
            )
        )
        table_high, table_low = ahead_ref[0, l], ahead_ref[1, l]
        bins = product(table_high, high) + product(table_low, high) + product(table_high, low)
        own_mid_ref[l] = bins[:, :LANES]
        mid_ref[l] = bins[:, LANES:]

    first, stop = start_ref[date], stop_ref[date]
    for m in range(TAPS):
        bin_index = lax.broadcasted_iota(jnp.int32, (inner, LANES), 0) + m * inner
        keep = (bin_index >= first) & (bin_index < stop)
        weight_ref[m] = jnp.where(keep, 1.0 / (TAPS * inner), 0.0)
    spectral(own_mid_ref, weight_ref, own_back_ref)
    for l in range(TAPS):
        signal = signal_of(own_back_ref, back_ref, l) * (1.0 / LOOKS)
        other = swap_halves(signal)
        mask = low_lanes(signal.shape)
        same_ref[l] = jnp.where(mask, signal, -other)
        cross_ref[l] = jnp.where(mask, other, signal)


def late_kernel(
    peers, late_ref, back_ref, mid_ref, weight_ref, same_ref, cross_ref, sec_ref, *refs
):
    out_refs = refs[:peers]
    total_ref, taps_ref, sum_ref = refs[peers:]
    me = lax.axis_index("line")
    inner = mid_ref.shape[1]
    few = sec_ref.shape[0] // TAPS
    rest = jnp.zeros((late_ref.shape[2] - 6 * few, LANES), jnp.bfloat16)
    for l in range(TAPS):
        span = pl.ds(l, few, stride=TAPS)
        values = sec_ref[span, :]
        high, low = split_pair(stacked(values, turned(values)))
        total_ref[l] = mid_ref[l] + product(late_ref[l], stacked(high, low, high, rest))
    spectral(total_ref, weight_ref, taps_ref)
    for half in range(2):
        same, cross = None, None
        for l in range(half * LOOKS, (half + 1) * LOOKS):
            signal = signal_of(taps_ref, back_ref, l)
            new_same, new_cross = same_ref[l] * signal, cross_ref[l] * signal
            same = new_same if same is None else same + new_same
            cross = new_cross if cross is None else cross + new_cross
        sum_ref[pl.ds(half, inner, stride=2), :] = same + swap_halves(cross)
    out_lines = 2 * inner // peers
    for q in range(peers):
        block = entry(RETURN[q - 1], me) if q else me
        base = pl.multiple_of(block_of(me, block, peers) * out_lines, 8)
        out_refs[q][...] = sum_ref[pl.ds(base, out_lines), :]


def unpack_kernel(peers, *refs):
    chunk_refs, (out_ref, held_ref) = refs[:peers], refs[peers:]
    me = lax.axis_index("line")
    for q in range(peers):
        held_ref[entry(senders(RETURN[q - 1]), me) if q else me] = chunk_refs[q][...]
    for pair in range(peers // 2):
        span = slice(pair * LANES, (pair + 1) * LANES)
        first, second = held_ref[2 * pair], held_ref[2 * pair + 1]
        mask = low_lanes(first.shape)
        out_ref[0, :, span] = jnp.where(mask, first, swap_halves(second))
        out_ref[1, :, span] = jnp.where(mask, swap_halves(first), second)


def packed_step(slc, band_start, band_stop):
    peers = lax.axis_size("line")
    chunk_lines = slc.shape[3]
    inner = peers * chunk_lines // TAPS
    out_lines = 2 * inner // peers
    f32 = jnp.float32
    vmem = pl.BlockSpec(memory_space=pltpu.VMEM)
    smem = pl.BlockSpec(memory_space=pltpu.SMEM)
    params = pltpu.CompilerParams(vmem_limit_bytes=16 * MIB)
    image = jnp.transpose(slc[0], (0, 2, 1))
    packed = pl.pallas_call(
        pack_kernel,
        out_shape=[jax.ShapeDtypeStruct((chunk_lines, LANES), f32)] * peers,
        in_specs=[vmem],
        out_specs=[vmem] * peers,
        compiler_params=pltpu.CompilerParams(vmem_limit_bytes=8 * MIB),
        name="pack",
    )(image)

    def exchange(values, row):
        return lax.ppermute(values, "line", list(enumerate(row)))

    def forward(values):
        return shifted(values, "date", -1)

    own = [
        exchange(values, EXCHANGE[q - 1]) if q else values
        for q, values in enumerate(packed)
    ]
    sec = [forward(values) for values in own]
    tables = [jnp.asarray(table) for table in host_tables(inner, 0, chunk_lines // TAPS)]
    ahead_table, back_table, late_table = pl.pallas_call(
        functools.partial(tables_kernel, len(tables)),
        out_shape=[jax.ShapeDtypeStruct(table.shape, table.dtype) for table in tables],
        in_specs=[vmem] * len(tables),
        out_specs=[vmem] * len(tables),
        compiler_params=params,
        name="tables",
    )(*tables)
    taps = jax.ShapeDtypeStruct((TAPS, inner, LANES), f32)
    plane = pltpu.VMEM((peers * chunk_lines, LANES), f32)
    middle, weight, same, cross = pl.pallas_call(
        functools.partial(early_kernel, peers),
        out_shape=[taps] * 4,
        in_specs=[smem, smem] + [vmem] * (2 * peers + 1),
        out_specs=[vmem] * 4,
        scratch_shapes=[plane] * 4 + [pltpu.VMEM(taps.shape, f32)] * 2,
        compiler_params=params,
        name="early",
    )(band_start, band_stop, ahead_table, back_table, *own, *sec[:-1])
    looked = pl.pallas_call(
        functools.partial(late_kernel, peers),
        out_shape=[jax.ShapeDtypeStruct((out_lines, LANES), f32)] * peers,
        in_specs=[vmem] * 7,
        out_specs=[vmem] * peers,
        scratch_shapes=[
            pltpu.VMEM(taps.shape, f32),
            pltpu.VMEM(taps.shape, f32),
            pltpu.VMEM((2 * inner, LANES), f32),
        ],
        compiler_params=params,
        name="late",
    )(late_table, back_table, middle, weight, same, cross, sec[-1])
    looked = [
        exchange(values, RETURN[q - 1]) if q else values
        for q, values in enumerate(looked)
    ]
    result = pl.pallas_call(
        functools.partial(unpack_kernel, peers),
        out_shape=jax.ShapeDtypeStruct((2, out_lines, slc.shape[2]), f32),
        in_specs=[vmem] * peers,
        out_specs=vmem,
        scratch_shapes=[pltpu.VMEM((peers, out_lines, LANES), f32)],
        compiler_params=pltpu.CompilerParams(vmem_limit_bytes=8 * MIB),
        name="unpack",
    )(*looked)
    return jnp.transpose(result, (0, 2, 1))[None]


def packs(mesh, slc):
    peers = mesh.shape["line"]
    columns = slc.shape[2] // mesh.shape["stack"] // peers
    chunk_lines = slc.shape[3] // peers
    inner = slc.shape[3] // TAPS
    return (
        columns == HALF
        and all(peers == len(row) for row in EXCHANGE)
        and chunk_lines % (16 * TAPS) == 0
        and inner % LANES == 0
        and inner <= 4 * LANES
    )


def solution(mesh):
    specs = dict(
        mesh=mesh,
        in_specs=(P("date", None, "stack", "line"), P(), P()),
        out_specs=P("date", None, "stack", "line"),
        check_vma=False,
    )

    def whole(slc, band_start, band_stop):
        if not packs(mesh, slc):
            return jax.shard_map(general_shards, **specs)(slc, band_start, band_stop)
        step = jax.shard_map(packed_step, **specs)
        return step(slc, band_start, band_stop)

    return whole
```

```python
import functools
import math

import jax
import jax.numpy as jnp
import numpy as np
from jax import lax
from jax.experimental import pallas as pl
from jax.experimental.pallas import tpu as pltpu
from jax.sharding import PartitionSpec as P


LOOKS = 5
TAPS = 2 * LOOKS
EXCHANGE = ((3, 2, 1, 0), (1, 0, 3, 2), (2, 3, 0, 1))
RETURN = ((2, 3, 0, 1), (3, 2, 1, 0), (1, 0, 3, 2))
LANES = 128
MIB = 1 << 20
HALF = LANES // 2


HIGHEST_PRECISION = lax.Precision.HIGHEST


def shifted(shard, axis, by):
    size = lax.axis_size(axis)
    return lax.ppermute(shard, axis, [(i, (i + by) % size) for i in range(size)])


def phase_table(count, sign_value):
    index_row = jnp.arange(count, dtype=jnp.int32)
    wrapped = index_row[:, None] * index_row[None, :] % count
    angle_all = 2.0 * math.pi / count * wrapped.astype(jnp.float32)
    return (jnp.cos(angle_all), sign_value * jnp.sin(angle_all))


def twiddle_table(outer, inner, sign_value):
    outer_row = jnp.arange(outer, dtype=jnp.int32)
    inner_row = jnp.arange(inner, dtype=jnp.int32)
    wrapped = outer_row[:, None] * inner_row[None, :] % (outer * inner)
    angle_all = 2.0 * math.pi / (outer * inner) * wrapped.astype(jnp.float32)
    return (jnp.cos(angle_all), sign_value * jnp.sin(angle_all))


def left_product(table_real, table_imag, data_real, data_imag):

    def single(table, data):
        return jnp.einsum("ka,cab->ckb", table, data, precision=HIGHEST_PRECISION)

    return (
        single(table_real, data_real) - single(table_imag, data_imag),
        single(table_real, data_imag) + single(table_imag, data_real),
    )


def right_product(data_real, data_imag, table_real, table_imag):

    def single(data, table):
        return jnp.einsum("ckb,bm->ckm", data, table, precision=HIGHEST_PRECISION)

    return (
        single(data_real, table_real) - single(data_imag, table_imag),
        single(data_imag, table_real) + single(data_real, table_imag),
    )


def forward_dft(data_real, data_imag):
    outer = data_real.shape[1]
    inner = data_real.shape[2]
    outer_real, outer_imag = phase_table(outer, -1.0)
    first_real, first_imag = left_product(outer_real, outer_imag, data_real, data_imag)
    twist_real, twist_imag = twiddle_table(outer, inner, -1.0)
    turned_real = first_real * twist_real - first_imag * twist_imag
    turned_imag = first_real * twist_imag + first_imag * twist_real
    inner_real, inner_imag = phase_table(inner, -1.0)
    return right_product(turned_real, turned_imag, inner_real, inner_imag)


def inverse_dft(data_real, data_imag):
    outer = data_real.shape[1]
    inner = data_real.shape[2]
    inner_real, inner_imag = phase_table(inner, 1.0)
    first_real, first_imag = right_product(data_real, data_imag, inner_real, inner_imag)
    twist_real, twist_imag = twiddle_table(outer, inner, 1.0)
    turned_real = first_real * twist_real - first_imag * twist_imag
    turned_imag = first_real * twist_imag + first_imag * twist_real
    outer_real, outer_imag = phase_table(outer, 1.0)
    result_real, result_imag = left_product(outer_real, outer_imag, turned_real, turned_imag)
    scale = 1.0 / (outer * inner)
    return (result_real * scale, result_imag * scale)


def conj_product(ref_real, ref_imag, sec_real, sec_imag):
    return (ref_real * sec_real + ref_imag * sec_imag, ref_imag * sec_real - ref_real * sec_imag)


def look_mean(values):
    return values.reshape(values.shape[0], values.shape[1] // LOOKS, LOOKS).sum(axis=-1) * (
        1.0 / LOOKS
    )


def general_shards(slc, band_start, band_stop):
    own_image = slc[0]
    line_lines = own_image.shape[2]
    turned = lax.all_to_all(own_image, "line", split_axis=1, concat_axis=2, tiled=True)
    columns = turned.shape[1]
    outer = lax.axis_size("line")
    lines_all = outer * line_lines
    blocks = turned.reshape(2, columns, outer, line_lines)
    spec_real, spec_imag = forward_dft(blocks[0], blocks[1])
    spectrum = jnp.stack([spec_real, spec_imag], axis=0)
    date_index = lax.axis_index("date")
    my_start = lax.dynamic_slice_in_dim(band_start, date_index, 1)[0]
    my_end = lax.dynamic_slice_in_dim(band_stop, date_index, 1)[0]
    bin_index = (
        jnp.arange(outer, dtype=jnp.int32)[:, None]
        + outer * jnp.arange(line_lines, dtype=jnp.int32)[None, :]
    )
    keep_mask = ((bin_index >= my_start) & (bin_index < my_end)).astype(jnp.float32)
    partner = shifted(spectrum, "date", -1)
    ref_spec = spectrum * keep_mask
    sec_spec = partner * keep_mask
    both_real, both_imag = inverse_dft(
        jnp.concatenate([ref_spec[0], sec_spec[0]], axis=0),
        jnp.concatenate([ref_spec[1], sec_spec[1]], axis=0),
    )
    ref_real = both_real[:columns].reshape(columns, lines_all)
    ref_imag = both_imag[:columns].reshape(columns, lines_all)
    sec_real = both_real[columns:].reshape(columns, lines_all)
    sec_imag = both_imag[columns:].reshape(columns, lines_all)
    prod_real, prod_imag = conj_product(ref_real, ref_imag, sec_real, sec_imag)
    looked = jnp.stack([look_mean(prod_real), look_mean(prod_imag)], axis=0)
    result = lax.all_to_all(looked, "line", split_axis=2, concat_axis=1, tiled=True)
    return result[None]


def split_pair(values):
    high = values.astype(jnp.bfloat16)
    low = (values - high.astype(jnp.float32)).astype(jnp.bfloat16)
    return high, low


@functools.lru_cache(maxsize=None)
def host_tables(inner, first_step, few):
    lines_all = TAPS * inner
    bins, steps, taps = np.arange(inner), np.arange(inner), np.arange(TAPS)
    turns = bins[None, :, None] * (TAPS * steps[None, None, :] + taps[:, None, None]) % lines_all
    angle = 2.0 * np.pi / lines_all * turns
    cos, sin = np.cos(angle), np.sin(angle)

    def halves(table):
        high = table.astype(jnp.bfloat16)
        low = (table - high.astype(np.float64)).astype(jnp.bfloat16)
        return high, low

    ahead = halves(np.concatenate([cos, sin], axis=2))
    swapped = [np.swapaxes(table, 1, 2) for table in (cos, -sin)]
    back = halves(np.concatenate(swapped, axis=2))
    part = slice(first_step, first_step + few)
    high, low = halves(np.concatenate([cos[:, :, part], sin[:, :, part]], axis=2))
    late = np.concatenate([high, high, low], axis=2)
    late = np.pad(late, ((0, 0), (0, 0), (0, -late.shape[2] % LANES)))
    return np.stack(ahead), np.stack(back), late


def low_lanes(shape):
    return lax.broadcasted_iota(jnp.int32, shape, len(shape) - 1) < HALF


def swap_halves(values):
    return pltpu.roll(values, HALF, values.ndim - 1)


def turned(values):
    other = swap_halves(values)
    return jnp.where(low_lanes(values.shape), other, -other)


def entry(row, me):
    code = sum(value << (4 * place) for place, value in enumerate(row))
    return jnp.bitwise_and(jnp.right_shift(jnp.int32(code), 4 * me), 15)


def senders(row):
    return tuple(row.index(place) for place in range(len(row)))


def pack_kernel(image_ref, *chunk_refs):
    me = lax.axis_index("line")
    peers = len(chunk_refs) - 1
    for q in range(peers):
        block = entry(EXCHANGE[q - 1], me) if q else me
        lane = pl.multiple_of(block // 2 * LANES, LANES)
        side = block % 2
        stay = image_ref[side, :, pl.ds(lane, LANES)]
        move = image_ref[1 - side, :, pl.ds(lane, LANES)]
        half = lax.broadcasted_iota(jnp.int32, stay.shape, 1) // HALF
        value = jnp.where(half == side, stay, swap_halves(move))
        if q < peers - 1:
            chunk_refs[q][...] = value
        else:
            cut = value.shape[0] // 2
            chunk_refs[q][...], chunk_refs[q + 1][...] = value[:cut], value[cut:]


COS1, COS2 = math.cos(2.0 * math.pi / 5), math.cos(4.0 * math.pi / 5)
SIN1, SIN2 = math.sin(2.0 * math.pi / 5), math.sin(4.0 * math.pi / 5)


def five_point(x, sign):
    unit = jnp.where(low_lanes(x[0].shape), sign, -sign)
    sin1, sin2 = SIN1 * unit, SIN2 * unit
    sum1, sum2 = x[1] + x[4], x[2] + x[3]
    dif1, dif2 = x[1] - x[4], x[2] - x[3]
    even1 = x[0] + COS1 * sum1 + COS2 * sum2
    even2 = x[0] + COS2 * sum1 + COS1 * sum2
    odd1 = swap_halves(sin1 * dif1 + sin2 * dif2)
    odd2 = swap_halves(sin2 * dif1 - sin1 * dif2)
    return [x[0] + sum1 + sum2, even1 + odd1, even2 + odd2, even2 - odd2, even1 - odd1]


def ten_point(x, sign):
    first = [x[2 * b % TAPS] for b in range(LOOKS)]
    other = [x[(LOOKS + 2 * b) % TAPS] for b in range(LOOKS)]
    even = five_point([p + q for p, q in zip(first, other)], sign)
    odd = five_point([p - q for p, q in zip(first, other)], sign)
    return [(odd if m % 2 else even)[m % LOOKS] for m in range(TAPS)]


def block_of(me, block, peers):
    return (block - entry(senders(EXCHANGE[-1]), me)) % peers


def product(table, data):
    return jnp.dot(table, data, preferred_element_type=jnp.float32)


def stacked(*values):
    return jnp.concatenate(values, axis=0)


def beside(*values):
    return jnp.concatenate(values, axis=1)


def spectral(mid_ref, weight_ref, back_ref):
    rows = 8

    def block(step, carry):
        span = pl.ds(pl.multiple_of(step * rows, rows), rows)
        x = ten_point([mid_ref[l, span, :] for l in range(TAPS)], -1.0)
        x = ten_point([x[m] * weight_ref[m, span, :] for m in range(TAPS)], 1.0)
        for l in range(TAPS):
            back_ref[l, span, :] = x[l]
        return carry

    lax.fori_loop(0, mid_ref.shape[1] // rows, block, 0, unroll=True)


def signal_of(mid_ref, back_ref, l):
    values = mid_ref[l]
    high, low = split_pair(stacked(values, turned(values)))
    both = beside(high, low)
    signal = product(back_ref[0, l], both) + product(back_ref[1, l], both)
    return signal[:, :LANES] + signal[:, LANES:]


def tables_kernel(count, *refs):
    for source, target in zip(refs[:count], refs[count:]):
        target[...] = source[...]


def weights_kernel(start_ref, stop_ref, weight_ref):
    taps, inner = weight_ref.shape[:2]
    date = lax.axis_index("date")
    start, stop = start_ref[date], stop_ref[date]
    for m in range(taps):
        bin_index = lax.broadcasted_iota(jnp.int32, (inner, LANES), 0) + m * inner
        keep = (bin_index >= start) & (bin_index < stop)
        weight_ref[m] = jnp.where(keep, 1.0 / (taps * inner), 0.0)


def early_kernel(peers, ahead_ref, back_ref, weight_ref, *refs):
    own_refs, sec_refs = refs[: peers + 1], refs[peers + 1 : 2 * peers]
    mid_ref, same_ref, cross_ref = refs[2 * peers : 2 * peers + 3]
    own_ref, own_turned_ref, sec_ref, sec_turned_ref = refs[2 * peers + 3 : -2]
    own_mid_ref, own_back_ref = refs[-2:]
    me = lax.axis_index("line")
    lines = own_ref.shape[0] // peers
    inner = own_ref.shape[0] // TAPS
    for q in range(peers):
        block = entry(senders(EXCHANGE[q - 1]), me) if q else me
        span = pl.ds(pl.multiple_of(block_of(me, block, peers) * lines, 8), lines)
        own = own_refs[q][...] if q < peers - 1 else stacked(own_refs[q][...], own_refs[q + 1][...])
        own_ref[span, :] = own
        own_turned_ref[span, :] = turned(own)
        if q == peers - 1:
            sec_ref[span, :] = jnp.zeros((lines, LANES), jnp.float32)
            sec_turned_ref[span, :] = jnp.zeros((lines, LANES), jnp.float32)
        else:
            sec = sec_refs[q][...]
            sec_ref[span, :] = sec
            sec_turned_ref[span, :] = turned(sec)
    for l in range(TAPS):
        span = pl.ds(l, inner, stride=TAPS)
        high, low = split_pair(
            stacked(
                beside(own_ref[span, :], sec_ref[span, :]),
                beside(own_turned_ref[span, :], sec_turned_ref[span, :]),
            )
        )
        table_high, table_low = ahead_ref[0, l], ahead_ref[1, l]
        bins = product(table_high, high) + product(table_low, high) + product(table_high, low)
        own_mid_ref[l] = bins[:, :LANES]
        mid_ref[l] = bins[:, LANES:]

    spectral(own_mid_ref, weight_ref, own_back_ref)
    for l in range(TAPS):
        signal = signal_of(own_back_ref, back_ref, l) * (1.0 / LOOKS)
        other = swap_halves(signal)
        mask = low_lanes(signal.shape)
        same_ref[l] = jnp.where(mask, signal, -other)
        cross_ref[l] = jnp.where(mask, other, signal)


def late_kernel(
    peers, late_ref, back_ref, mid_ref, weight_ref, same_ref, cross_ref, sec_ref, rest_ref, *refs
):
    out_refs = refs[:peers]
    total_ref, taps_ref, sum_ref = refs[peers:]
    me = lax.axis_index("line")
    inner = mid_ref.shape[1]
    few = 2 * sec_ref.shape[0] // TAPS
    rest = jnp.zeros((late_ref.shape[2] - 6 * few, LANES), jnp.bfloat16)
    for l in range(TAPS):
        span = pl.ds(l, few // 2, stride=TAPS)
        values = stacked(sec_ref[span, :], rest_ref[span, :])
        high, low = split_pair(stacked(values, turned(values)))
        total_ref[l] = mid_ref[l] + product(late_ref[l], stacked(high, low, high, rest))
    spectral(total_ref, weight_ref, taps_ref)
    for half in range(2):
        same, cross = None, None
        for l in range(half * LOOKS, (half + 1) * LOOKS):
            signal = signal_of(taps_ref, back_ref, l)
            new_same, new_cross = same_ref[l] * signal, cross_ref[l] * signal
            same = new_same if same is None else same + new_same
            cross = new_cross if cross is None else cross + new_cross
        sum_ref[pl.ds(half, inner, stride=2), :] = same + swap_halves(cross)
    out_lines = 2 * inner // peers
    for q in range(peers):
        block = entry(RETURN[q - 1], me) if q else me
        base = pl.multiple_of(block_of(me, block, peers) * out_lines, 8)
        out_refs[q][...] = sum_ref[pl.ds(base, out_lines), :]


def unpack_kernel(peers, *refs):
    chunk_refs, (out_ref, held_ref) = refs[:peers], refs[peers:]
    me = lax.axis_index("line")
    for q in range(peers):
        held_ref[entry(senders(RETURN[q - 1]), me) if q else me] = chunk_refs[q][...]
    for pair in range(peers // 2):
        span = slice(pair * LANES, (pair + 1) * LANES)
        first, second = held_ref[2 * pair], held_ref[2 * pair + 1]
        mask = low_lanes(first.shape)
        out_ref[0, :, span] = jnp.where(mask, first, swap_halves(second))
        out_ref[1, :, span] = jnp.where(mask, swap_halves(first), second)


def packed_step(slc, band_start, band_stop):
    peers = lax.axis_size("line")
    chunk_lines = slc.shape[3]
    inner = peers * chunk_lines // TAPS
    out_lines = 2 * inner // peers
    f32 = jnp.float32
    vmem = pl.BlockSpec(memory_space=pltpu.VMEM)
    smem = pl.BlockSpec(memory_space=pltpu.SMEM)
    params = pltpu.CompilerParams(vmem_limit_bytes=16 * MIB)
    image = jnp.transpose(slc[0], (0, 2, 1))
    chunk = jax.ShapeDtypeStruct((chunk_lines, LANES), f32)
    part = jax.ShapeDtypeStruct((chunk_lines // 2, LANES), f32)
    packed = pl.pallas_call(
        pack_kernel,
        out_shape=[chunk] * (peers - 1) + [part] * 2,
        in_specs=[vmem],
        out_specs=[vmem] * (peers + 1),
        compiler_params=pltpu.CompilerParams(vmem_limit_bytes=8 * MIB),
        name="pack",
    )(image)

    def exchange(values, row):
        return lax.ppermute(values, "line", list(enumerate(row)))

    def forward(values):
        return shifted(values, "date", -1)

    own = [
        exchange(values, EXCHANGE[min(q, peers - 1) - 1]) if q else values
        for q, values in enumerate(packed)
    ]
    sec = [forward(values) for values in own]
    tables = [jnp.asarray(table) for table in host_tables(inner, 0, chunk_lines // TAPS)]
    taps = jax.ShapeDtypeStruct((TAPS, inner, LANES), f32)
    ahead_table, back_table, late_table = pl.pallas_call(
        functools.partial(tables_kernel, len(tables)),
        out_shape=[jax.ShapeDtypeStruct(table.shape, table.dtype) for table in tables],
        in_specs=[vmem] * len(tables),
        out_specs=[vmem] * len(tables),
        compiler_params=params,
        name="tables",
    )(*tables)
    weight = pl.pallas_call(
        weights_kernel,
        out_shape=taps,
        in_specs=[smem, smem],
        out_specs=vmem,
        compiler_params=params,
        name="weights",
    )(band_start, band_stop)
    plane = pltpu.VMEM((peers * chunk_lines, LANES), f32)
    middle, same, cross = pl.pallas_call(
        functools.partial(early_kernel, peers),
        out_shape=[taps] * 3,
        in_specs=[vmem] * (2 * peers + 3),
        out_specs=[vmem] * 3,
        scratch_shapes=[plane] * 4 + [pltpu.VMEM(taps.shape, f32)] * 2,
        compiler_params=params,
        name="early",
    )(ahead_table, back_table, weight, *own, *sec[:-2])
    looked = pl.pallas_call(
        functools.partial(late_kernel, peers),
        out_shape=[jax.ShapeDtypeStruct((out_lines, LANES), f32)] * peers,
        in_specs=[vmem] * 8,
        out_specs=[vmem] * peers,
        scratch_shapes=[
            pltpu.VMEM(taps.shape, f32),
            pltpu.VMEM(taps.shape, f32),
            pltpu.VMEM((2 * inner, LANES), f32),
        ],
        compiler_params=params,
        name="late",
    )(late_table, back_table, middle, weight, same, cross, *sec[-2:])
    looked = [exchange(values, RETURN[q - 1]) if q else values for q, values in enumerate(looked)]
    result = pl.pallas_call(
        functools.partial(unpack_kernel, peers),
        out_shape=jax.ShapeDtypeStruct((2, out_lines, slc.shape[2]), f32),
        in_specs=[vmem] * peers,
        out_specs=vmem,
        scratch_shapes=[pltpu.VMEM((peers, out_lines, LANES), f32)],
        compiler_params=pltpu.CompilerParams(vmem_limit_bytes=8 * MIB),
        name="unpack",
    )(*looked)
    return jnp.transpose(result, (0, 2, 1))[None]


def packs(mesh, slc):
    peers = mesh.shape["line"]
    columns = slc.shape[2] // mesh.shape["stack"] // peers
    chunk_lines = slc.shape[3] // peers
    inner = slc.shape[3] // TAPS
    return (
        columns == HALF
        and all(peers == len(row) for row in EXCHANGE)
        and chunk_lines % (32 * TAPS) == 0
        and inner % LANES == 0
        and inner <= 4 * LANES
    )


def solution(mesh):
    specs = dict(
        mesh=mesh,
        in_specs=(P("date", None, "stack", "line"), P(), P()),
        out_specs=P("date", None, "stack", "line"),
        check_vma=False,
    )

    def whole(slc, band_start, band_stop):
        if not packs(mesh, slc):
            return jax.shard_map(general_shards, **specs)(slc, band_start, band_stop)
        step = jax.shard_map(packed_step, **specs)
        return step(slc, band_start, band_stop)

    return whole
```

```python
import functools
import math

import jax
import jax.numpy as jnp
import numpy as np
from jax import lax
from jax.experimental import pallas as pl
from jax.experimental.pallas import tpu as pltpu
from jax.sharding import PartitionSpec as P


LOOKS = 5
TAPS = 2 * LOOKS
EXCHANGE = ((3, 2, 1, 0), (1, 0, 3, 2), (2, 3, 0, 1))
RETURN = ((2, 3, 0, 1), (3, 2, 1, 0), (1, 0, 3, 2))
LANES = 128
MIB = 1 << 20
HALF = LANES // 2


HIGHEST_PRECISION = lax.Precision.HIGHEST


def shifted(shard, axis, by):
    size = lax.axis_size(axis)
    return lax.ppermute(shard, axis, [(i, (i + by) % size) for i in range(size)])


def phase_table(count, sign_value):
    index_row = jnp.arange(count, dtype=jnp.int32)
    wrapped = index_row[:, None] * index_row[None, :] % count
    angle_all = 2.0 * math.pi / count * wrapped.astype(jnp.float32)
    return (jnp.cos(angle_all), sign_value * jnp.sin(angle_all))


def twiddle_table(outer, inner, sign_value):
    outer_row = jnp.arange(outer, dtype=jnp.int32)
    inner_row = jnp.arange(inner, dtype=jnp.int32)
    wrapped = outer_row[:, None] * inner_row[None, :] % (outer * inner)
    angle_all = 2.0 * math.pi / (outer * inner) * wrapped.astype(jnp.float32)
    return (jnp.cos(angle_all), sign_value * jnp.sin(angle_all))


def left_product(table_real, table_imag, data_real, data_imag):

    def single(table, data):
        return jnp.einsum("ka,cab->ckb", table, data, precision=HIGHEST_PRECISION)

    return (
        single(table_real, data_real) - single(table_imag, data_imag),
        single(table_real, data_imag) + single(table_imag, data_real),
    )


def right_product(data_real, data_imag, table_real, table_imag):

    def single(data, table):
        return jnp.einsum("ckb,bm->ckm", data, table, precision=HIGHEST_PRECISION)

    return (
        single(data_real, table_real) - single(data_imag, table_imag),
        single(data_imag, table_real) + single(data_real, table_imag),
    )


def forward_dft(data_real, data_imag):
    outer = data_real.shape[1]
    inner = data_real.shape[2]
    outer_real, outer_imag = phase_table(outer, -1.0)
    first_real, first_imag = left_product(outer_real, outer_imag, data_real, data_imag)
    twist_real, twist_imag = twiddle_table(outer, inner, -1.0)
    turned_real = first_real * twist_real - first_imag * twist_imag
    turned_imag = first_real * twist_imag + first_imag * twist_real
    inner_real, inner_imag = phase_table(inner, -1.0)
    return right_product(turned_real, turned_imag, inner_real, inner_imag)


def inverse_dft(data_real, data_imag):
    outer = data_real.shape[1]
    inner = data_real.shape[2]
    inner_real, inner_imag = phase_table(inner, 1.0)
    first_real, first_imag = right_product(data_real, data_imag, inner_real, inner_imag)
    twist_real, twist_imag = twiddle_table(outer, inner, 1.0)
    turned_real = first_real * twist_real - first_imag * twist_imag
    turned_imag = first_real * twist_imag + first_imag * twist_real
    outer_real, outer_imag = phase_table(outer, 1.0)
    result_real, result_imag = left_product(outer_real, outer_imag, turned_real, turned_imag)
    scale = 1.0 / (outer * inner)
    return (result_real * scale, result_imag * scale)


def conj_product(ref_real, ref_imag, sec_real, sec_imag):
    return (ref_real * sec_real + ref_imag * sec_imag, ref_imag * sec_real - ref_real * sec_imag)


def look_mean(values):
    return values.reshape(values.shape[0], values.shape[1] // LOOKS, LOOKS).sum(axis=-1) * (
        1.0 / LOOKS
    )


def general_shards(slc, band_start, band_stop):
    own_image = slc[0]
    line_lines = own_image.shape[2]
    turned = lax.all_to_all(own_image, "line", split_axis=1, concat_axis=2, tiled=True)
    columns = turned.shape[1]
    outer = lax.axis_size("line")
    lines_all = outer * line_lines
    blocks = turned.reshape(2, columns, outer, line_lines)
    spec_real, spec_imag = forward_dft(blocks[0], blocks[1])
    spectrum = jnp.stack([spec_real, spec_imag], axis=0)
    date_index = lax.axis_index("date")
    my_start = lax.dynamic_slice_in_dim(band_start, date_index, 1)[0]
    my_end = lax.dynamic_slice_in_dim(band_stop, date_index, 1)[0]
    bin_index = (
        jnp.arange(outer, dtype=jnp.int32)[:, None]
        + outer * jnp.arange(line_lines, dtype=jnp.int32)[None, :]
    )
    keep_mask = ((bin_index >= my_start) & (bin_index < my_end)).astype(jnp.float32)
    partner = shifted(spectrum, "date", -1)
    ref_spec = spectrum * keep_mask
    sec_spec = partner * keep_mask
    both_real, both_imag = inverse_dft(
        jnp.concatenate([ref_spec[0], sec_spec[0]], axis=0),
        jnp.concatenate([ref_spec[1], sec_spec[1]], axis=0),
    )
    ref_real = both_real[:columns].reshape(columns, lines_all)
    ref_imag = both_imag[:columns].reshape(columns, lines_all)
    sec_real = both_real[columns:].reshape(columns, lines_all)
    sec_imag = both_imag[columns:].reshape(columns, lines_all)
    prod_real, prod_imag = conj_product(ref_real, ref_imag, sec_real, sec_imag)
    looked = jnp.stack([look_mean(prod_real), look_mean(prod_imag)], axis=0)
    result = lax.all_to_all(looked, "line", split_axis=2, concat_axis=1, tiled=True)
    return result[None]


def split_pair(values):
    high = values.astype(jnp.bfloat16)
    low = (values - high.astype(jnp.float32)).astype(jnp.bfloat16)
    return high, low


@functools.lru_cache(maxsize=None)
def host_tables(inner, first_step, few):
    lines_all = TAPS * inner
    bins, steps, taps = np.arange(inner), np.arange(inner), np.arange(TAPS)
    turns = bins[None, :, None] * (TAPS * steps[None, None, :] + taps[:, None, None]) % lines_all
    angle = 2.0 * np.pi / lines_all * turns
    cos, sin = np.cos(angle), np.sin(angle)

    def halves(table):
        high = table.astype(jnp.bfloat16)
        low = (table - high.astype(np.float64)).astype(jnp.bfloat16)
        return high, low

    ahead = halves(np.concatenate([cos, sin], axis=2))
    swapped = [np.swapaxes(table, 1, 2) for table in (cos, -sin)]
    back = halves(np.concatenate(swapped, axis=2))
    part = slice(first_step, first_step + few)
    high, low = halves(np.concatenate([cos[:, :, part], sin[:, :, part]], axis=2))
    late = np.concatenate([high, high, low], axis=2)
    late = np.pad(late, ((0, 0), (0, 0), (0, -late.shape[2] % LANES)))
    return np.stack(ahead), np.stack(back), late


def low_lanes(shape):
    return lax.broadcasted_iota(jnp.int32, shape, len(shape) - 1) < HALF


def swap_halves(values):
    return pltpu.roll(values, HALF, values.ndim - 1)


def turned(values):
    other = swap_halves(values)
    return jnp.where(low_lanes(values.shape), other, -other)


def entry(row, me):
    code = sum(value << (4 * place) for place, value in enumerate(row))
    return jnp.bitwise_and(jnp.right_shift(jnp.int32(code), 4 * me), 15)


def senders(row):
    return tuple(row.index(place) for place in range(len(row)))


def pack_kernel(image_ref, *chunk_refs):
    me = lax.axis_index("line")
    peers = len(chunk_refs) - 1
    for q in range(peers):
        block = entry(EXCHANGE[q - 1], me) if q else me
        lane = pl.multiple_of(block // 2 * LANES, LANES)
        side = block % 2
        stay = image_ref[side, :, pl.ds(lane, LANES)]
        move = image_ref[1 - side, :, pl.ds(lane, LANES)]
        half = lax.broadcasted_iota(jnp.int32, stay.shape, 1) // HALF
        value = jnp.where(half == side, stay, swap_halves(move))
        if q < peers - 1:
            chunk_refs[q][...] = value
        else:
            cut = value.shape[0] // 2
            chunk_refs[q][...], chunk_refs[q + 1][...] = value[:cut], value[cut:]


COS1, COS2 = math.cos(2.0 * math.pi / 5), math.cos(4.0 * math.pi / 5)
SIN1, SIN2 = math.sin(2.0 * math.pi / 5), math.sin(4.0 * math.pi / 5)


def five_point(x, sign):
    unit = jnp.where(low_lanes(x[0].shape), sign, -sign)
    sin1, sin2 = SIN1 * unit, SIN2 * unit
    sum1, sum2 = x[1] + x[4], x[2] + x[3]
    dif1, dif2 = x[1] - x[4], x[2] - x[3]
    even1 = x[0] + COS1 * sum1 + COS2 * sum2
    even2 = x[0] + COS2 * sum1 + COS1 * sum2
    odd1 = swap_halves(sin1 * dif1 + sin2 * dif2)
    odd2 = swap_halves(sin2 * dif1 - sin1 * dif2)
    return [x[0] + sum1 + sum2, even1 + odd1, even2 + odd2, even2 - odd2, even1 - odd1]


def ten_point(x, sign):
    first = [x[2 * b % TAPS] for b in range(LOOKS)]
    other = [x[(LOOKS + 2 * b) % TAPS] for b in range(LOOKS)]
    even = five_point([p + q for p, q in zip(first, other)], sign)
    odd = five_point([p - q for p, q in zip(first, other)], sign)
    return [(odd if m % 2 else even)[m % LOOKS] for m in range(TAPS)]


def block_of(me, block, peers):
    return (block - entry(senders(EXCHANGE[-1]), me)) % peers


def product(table, data):
    return jnp.dot(table, data, preferred_element_type=jnp.float32)


def stacked(*values):
    return jnp.concatenate(values, axis=0)


def beside(*values):
    return jnp.concatenate(values, axis=1)


def spectral(mid_ref, weight_ref, back_ref):
    rows = 8

    def block(step, carry):
        span = pl.ds(pl.multiple_of(step * rows, rows), rows)
        x = ten_point([mid_ref[l, span, :] for l in range(TAPS)], -1.0)
        x = ten_point([x[m] * weight_ref[m, span, :] for m in range(TAPS)], 1.0)
        for l in range(TAPS):
            back_ref[l, span, :] = x[l]
        return carry

    lax.fori_loop(0, mid_ref.shape[1] // rows, block, 0, unroll=True)


def signal_of(mid_ref, back_ref, l):
    values = mid_ref[l]
    high, low = split_pair(stacked(values, turned(values)))
    both = beside(high, low)
    signal = product(back_ref[0, l], both) + product(back_ref[1, l], both)
    return signal[:, :LANES] + signal[:, LANES:]


def tables_kernel(count, *refs):
    for source, target in zip(refs[:count], refs[count:]):
        target[...] = source[...]


def weights_kernel(start_ref, stop_ref, weight_ref):
    taps, inner = weight_ref.shape[:2]
    date = lax.axis_index("date")
    start, stop = start_ref[date], stop_ref[date]
    for m in range(taps):
        bin_index = lax.broadcasted_iota(jnp.int32, (inner, LANES), 0) + m * inner
        keep = (bin_index >= start) & (bin_index < stop)
        weight_ref[m] = jnp.where(keep, 1.0 / (taps * inner), 0.0)


def place(peers, chunk_refs, place_ref, turned_ref):
    me = lax.axis_index("line")
    lines = place_ref.shape[0] // peers
    for q in range(peers):
        block = entry(senders(EXCHANGE[q - 1]), me) if q else me
        span = pl.ds(pl.multiple_of(block_of(me, block, peers) * lines, 8), lines)
        if q < len(chunk_refs):
            values = chunk_refs[q][...]
            place_ref[span, :], turned_ref[span, :] = values, turned(values)
        else:
            zeros = jnp.zeros((lines, LANES), jnp.float32)
            place_ref[span, :], turned_ref[span, :] = zeros, zeros


def bins_of(place_ref, turned_ref, ahead_ref, l):
    span = pl.ds(l, place_ref.shape[0] // TAPS, stride=TAPS)
    both = beside(*split_pair(stacked(place_ref[span, :], turned_ref[span, :])))
    bins = product(ahead_ref[0, l], both) + product(ahead_ref[1, l], both)
    return bins[:, :LANES] + bins[:, LANES:]


def last_bins_of(first_ref, rest_ref, late_ref, l):
    few = 2 * first_ref.shape[0] // TAPS
    span = pl.ds(l, few // 2, stride=TAPS)
    values = stacked(first_ref[span, :], rest_ref[span, :])
    high, low = split_pair(stacked(values, turned(values)))
    rest = jnp.zeros((late_ref.shape[2] - 6 * few, LANES), jnp.bfloat16)
    return product(late_ref[l], stacked(high, low, high, rest))


def first_kernel(peers, ahead_ref, *refs):
    own_refs, (mid_ref, place_ref, turned_ref) = refs[: peers - 1], refs[peers - 1 :]
    place(peers, own_refs, place_ref, turned_ref)
    for l in range(TAPS):
        mid_ref[l] = bins_of(place_ref, turned_ref, ahead_ref, l)


def early_kernel(
    peers, ahead_ref, back_ref, late_ref, weight_ref, first_ref, last_ref, rest_ref, *refs
):
    sec_refs = refs[: peers - 1]
    mid_ref, same_ref, cross_ref, place_ref, turned_ref, own_mid_ref, own_back_ref = refs[peers - 1 :]
    for l in range(TAPS):
        own_mid_ref[l] = first_ref[l] + last_bins_of(last_ref, rest_ref, late_ref, l)
    place(peers, sec_refs, place_ref, turned_ref)
    for l in range(TAPS):
        mid_ref[l] = bins_of(place_ref, turned_ref, ahead_ref, l)
    spectral(own_mid_ref, weight_ref, own_back_ref)
    for l in range(TAPS):
        signal = signal_of(own_back_ref, back_ref, l) * (1.0 / LOOKS)
        other = swap_halves(signal)
        mask = low_lanes(signal.shape)
        same_ref[l] = jnp.where(mask, signal, -other)
        cross_ref[l] = jnp.where(mask, other, signal)


def late_kernel(
    peers, late_ref, back_ref, mid_ref, weight_ref, same_ref, cross_ref, sec_ref, rest_ref, *refs
):
    out_refs = refs[:peers]
    total_ref, taps_ref, sum_ref = refs[peers:]
    me = lax.axis_index("line")
    inner = mid_ref.shape[1]
    for l in range(TAPS):
        total_ref[l] = mid_ref[l] + last_bins_of(sec_ref, rest_ref, late_ref, l)
    spectral(total_ref, weight_ref, taps_ref)
    for half in range(2):
        same, cross = None, None
        for l in range(half * LOOKS, (half + 1) * LOOKS):
            signal = signal_of(taps_ref, back_ref, l)
            new_same, new_cross = same_ref[l] * signal, cross_ref[l] * signal
            same = new_same if same is None else same + new_same
            cross = new_cross if cross is None else cross + new_cross
        sum_ref[pl.ds(half, inner, stride=2), :] = same + swap_halves(cross)
    out_lines = 2 * inner // peers
    for q in range(peers):
        block = entry(RETURN[q - 1], me) if q else me
        base = pl.multiple_of(block_of(me, block, peers) * out_lines, 8)
        out_refs[q][...] = sum_ref[pl.ds(base, out_lines), :]


def unpack_kernel(peers, *refs):
    chunk_refs, (out_ref, held_ref) = refs[:peers], refs[peers:]
    me = lax.axis_index("line")
    for q in range(peers):
        held_ref[entry(senders(RETURN[q - 1]), me) if q else me] = chunk_refs[q][...]
    for pair in range(peers // 2):
        span = slice(pair * LANES, (pair + 1) * LANES)
        first, second = held_ref[2 * pair], held_ref[2 * pair + 1]
        mask = low_lanes(first.shape)
        out_ref[0, :, span] = jnp.where(mask, first, swap_halves(second))
        out_ref[1, :, span] = jnp.where(mask, swap_halves(first), second)


def packed_step(slc, band_start, band_stop):
    peers = lax.axis_size("line")
    chunk_lines = slc.shape[3]
    inner = peers * chunk_lines // TAPS
    out_lines = 2 * inner // peers
    f32 = jnp.float32
    vmem = pl.BlockSpec(memory_space=pltpu.VMEM)
    smem = pl.BlockSpec(memory_space=pltpu.SMEM)
    params = pltpu.CompilerParams(vmem_limit_bytes=16 * MIB)
    image = jnp.transpose(slc[0], (0, 2, 1))
    chunk = jax.ShapeDtypeStruct((chunk_lines, LANES), f32)
    part = jax.ShapeDtypeStruct((chunk_lines // 2, LANES), f32)
    packed = pl.pallas_call(
        pack_kernel,
        out_shape=[chunk] * (peers - 1) + [part] * 2,
        in_specs=[vmem],
        out_specs=[vmem] * (peers + 1),
        compiler_params=pltpu.CompilerParams(vmem_limit_bytes=8 * MIB),
        name="pack",
    )(image)

    def exchange(values, row):
        return lax.ppermute(values, "line", list(enumerate(row)))

    def forward(values):
        return shifted(values, "date", -1)

    own = [
        exchange(values, EXCHANGE[min(q, peers - 1) - 1]) if q else values
        for q, values in enumerate(packed)
    ]
    sec = [forward(values) for values in own]
    tables = [jnp.asarray(table) for table in host_tables(inner, 0, chunk_lines // TAPS)]
    taps = jax.ShapeDtypeStruct((TAPS, inner, LANES), f32)
    ahead_table, back_table, late_table = pl.pallas_call(
        functools.partial(tables_kernel, len(tables)),
        out_shape=[jax.ShapeDtypeStruct(table.shape, table.dtype) for table in tables],
        in_specs=[vmem] * len(tables),
        out_specs=[vmem] * len(tables),
        compiler_params=params,
        name="tables",
    )(*tables)
    weight = pl.pallas_call(
        weights_kernel,
        out_shape=taps,
        in_specs=[smem, smem],
        out_specs=vmem,
        compiler_params=params,
        name="weights",
    )(band_start, band_stop)
    plane = pltpu.VMEM((peers * chunk_lines, LANES), f32)
    first = pl.pallas_call(
        functools.partial(first_kernel, peers),
        out_shape=taps,
        in_specs=[vmem] * peers,
        out_specs=vmem,
        scratch_shapes=[plane] * 2,
        compiler_params=params,
        name="first",
    )(ahead_table, *own[:-2])
    middle, same, cross = pl.pallas_call(
        functools.partial(early_kernel, peers),
        out_shape=[taps] * 3,
        in_specs=[vmem] * (peers + 6),
        out_specs=[vmem] * 3,
        scratch_shapes=[plane] * 2 + [pltpu.VMEM(taps.shape, f32)] * 2,
        compiler_params=params,
        name="early",
    )(ahead_table, back_table, late_table, weight, first, *own[-2:], *sec[:-2])
    looked = pl.pallas_call(
        functools.partial(late_kernel, peers),
        out_shape=[jax.ShapeDtypeStruct((out_lines, LANES), f32)] * peers,
        in_specs=[vmem] * 8,
        out_specs=[vmem] * peers,
        scratch_shapes=[
            pltpu.VMEM(taps.shape, f32),
            pltpu.VMEM(taps.shape, f32),
            pltpu.VMEM((2 * inner, LANES), f32),
        ],
        compiler_params=params,
        name="late",
    )(late_table, back_table, middle, weight, same, cross, *sec[-2:])
    looked = [exchange(values, RETURN[q - 1]) if q else values for q, values in enumerate(looked)]
    result = pl.pallas_call(
        functools.partial(unpack_kernel, peers),
        out_shape=jax.ShapeDtypeStruct((2, out_lines, slc.shape[2]), f32),
        in_specs=[vmem] * peers,
        out_specs=vmem,
        scratch_shapes=[pltpu.VMEM((peers, out_lines, LANES), f32)],
        compiler_params=pltpu.CompilerParams(vmem_limit_bytes=8 * MIB),
        name="unpack",
    )(*looked)
    return jnp.transpose(result, (0, 2, 1))[None]


def packs(mesh, slc):
    peers = mesh.shape["line"]
    columns = slc.shape[2] // mesh.shape["stack"] // peers
    chunk_lines = slc.shape[3] // peers
    inner = slc.shape[3] // TAPS
    return (
        columns == HALF
        and all(peers == len(row) for row in EXCHANGE)
        and chunk_lines % (32 * TAPS) == 0
        and inner % LANES == 0
        and inner <= 4 * LANES
    )


def solution(mesh):
    specs = dict(
        mesh=mesh,
        in_specs=(P("date", None, "stack", "line"), P(), P()),
        out_specs=P("date", None, "stack", "line"),
        check_vma=False,
    )

    def whole(slc, band_start, band_stop):
        if not packs(mesh, slc):
            return jax.shard_map(general_shards, **specs)(slc, band_start, band_stop)
        step = jax.shard_map(packed_step, **specs)
        return step(slc, band_start, band_stop)

    return whole
```
